512 devices in a mesh: gx: 16 (over y_lo, z), gy: 4 (over x), col: 8 (over y_hi, core).
Axes of the slice: x: 4, y: 8 (y_hi: 4, y_lo: 2; y = y_hi * 2 + y_lo), z: 8, core: 2. Of those that a mesh axis runs over, the one named last changes fastest.
Arguments:
- fields: bfloat16 [8, 128, 128, 32, 128], P('col', 'gx', 'gy'), may hold values from -6 to 6
- spectral: bfloat16 [1, 16, 16, 2, 32, 32, 16], P(None, 'gx', 'gy', None, None, 'col'), may hold values from -0.75 to 0.75
- skip_weight: bfloat16 [1, 32, 32], replicated, may hold values from -1 to 1
- skip_bias: float32 [1, 32], replicated, may hold values from -3 to 3
- norm_gain: float32 [1, 32], replicated, may hold values from 0.5 to 1.5
- norm_shift: float32 [1, 32], replicated, may hold values from -3 to 3
Outputs:
- activations: bfloat16 [8, 128, 128, 32, 128], P('col', 'gx', 'gy')
The draws below stay inside these ranges and needn't reach their ends.
All inputs are finite; a program needn't handle non-finite values.
Results may differ from the reference program's by a relative error of at most 0.012.
Values may be sent and summed in bfloat16 or wider, within the bound.
No kernel may reach another device: no remote copies, remote signals or barrier semaphores. Data moves between devices by JAX's collectives and lax.ppermute only.
A program may use at most 64 MiB of HBM per device.

```python
import math
import jax
import jax.numpy as jnp
from jax import lax

X = 128
Y = 128
Z = 128
C = 32
MX = 16
MY = 16
MZ = 16
LAYERS = 1
SAMPLES = 8


def block_levels(own_key, shape, split, low, largest):
    def one(dim, shards_of):
        draws = jax.random.uniform(jax.random.fold_in(jax.random.fold_in(own_key, 6), dim), (shards_of,), jnp.float32, low / len(split), largest / len(split))
        return jnp.repeat(jnp.exp(draws), shape[dim] // shards_of).reshape((-1,) + (1,) * (len(shape) - dim - 1))

    level = one(*split[0])
    for cut in split[1:]:
        level = level * one(*cut)
    return level


def scatter_about(stream_key, dims, scale, bound, split=(), kind=jnp.bfloat16):
    gain = block_levels(stream_key, dims, split, -0.22, 0.18) if split else 1.0
    array = jax.random.normal(stream_key, dims, jnp.float32) * scale * gain
    return jnp.minimum(jnp.maximum(array, -bound), bound).astype(kind)


def setup_inputs(seed: int = 0) -> dict:
    keys = jax.random.split(jax.random.key(seed), 7)
    fields = scatter_about(keys[0], (SAMPLES, X, Y, C, Z), 1.0, 6.0, ((0, 8), (1, 16), (2, 4)))
    spectral = scatter_about(keys[1], (LAYERS, MX, MY, 2, C, C, MZ), (2 * C) ** -0.5, 0.75, ((1, 16), (2, 4), (5, 8)))
    skip_weight = scatter_about(keys[2], (LAYERS, C, C), C ** -0.5, 1.0)
    skip_bias = scatter_about(keys[3], (LAYERS, C), 0.5, 3.0, (), jnp.float32)
    norm_gain = jnp.clip(jax.random.uniform(keys[4], (LAYERS, C), jnp.float32, 0.5, 1.5), 0.5, 1.5)
    norm_shift = scatter_about(keys[5], (LAYERS, C), 0.5, 3.0, (), jnp.float32)
    return dict(fields=fields, spectral=spectral, skip_weight=skip_weight, skip_bias=skip_bias, norm_gain=norm_gain, norm_shift=norm_shift)


norm_eps = 1e-05

def signed_freqs(count):
    index = jnp.arange(count, dtype=jnp.int32)
    return jnp.where(index < count // 2, index, index - count)

def angles(positions, frequency, length):
    turn_count = positions[:, None] * frequency[None, :] % length
    return turn_count.astype(jnp.float32) * (2.0 * math.pi / length)

def forward_table(positions, frequency, length, factor):
    phase_angle = angles(positions, frequency, length)
    cosine = jnp.cos(phase_angle) * factor
    sine_part = jnp.sin(phase_angle) * factor
    from_real = jnp.stack([cosine, -sine_part], axis=-1)
    from_imag = jnp.stack([sine_part, cosine], axis=-1)
    return jnp.stack([from_real, from_imag], axis=1)

def inverse_table(frequency, positions, length):
    phase_angle = angles(positions, frequency, length).T
    cosine = jnp.cos(phase_angle)
    sine_part = jnp.sin(phase_angle)
    from_real = jnp.stack([cosine, sine_part], axis=-1)
    from_imag = jnp.stack([-sine_part, cosine], axis=-1)
    return jnp.stack([from_real, from_imag], axis=1)

def depth_tables(length, count):
    frequency = jnp.arange(count, dtype=jnp.int32)
    phase_angle = angles(jnp.arange(length, dtype=jnp.int32), frequency, length)
    forward = jnp.concatenate([jnp.cos(phase_angle), -jnp.sin(phase_angle)], axis=1)
    backward = jnp.concatenate([jnp.cos(phase_angle).T, -jnp.sin(phase_angle).T], axis=0)
    return (forward.astype(jnp.bfloat16), backward.astype(jnp.bfloat16))

def mix_modes(spectrum, weight):

    def contract(left, right):
        return jnp.einsum('abcz,abcdz->abdz', left, right, preferred_element_type=jnp.float32, precision=lax.Precision.HIGHEST)
    real_in = spectrum[:, :, :, 0]
    imag_in = spectrum[:, :, :, 1]
    real_weight = weight[:, :, 0]
    imag_weight = weight[:, :, 1]
    real_out = contract(real_in, real_weight) - contract(imag_in, imag_weight)
    imag_out = contract(real_in, imag_weight) + contract(imag_in, real_weight)
    return jnp.stack([real_out, imag_out], axis=3)

def finish(spectral_part, skip_part, offset, scaling, shift_term):
    pre_norm = spectral_part + skip_part + offset[:, None]
    centre = lax.optimization_barrier(jnp.mean(pre_norm, axis=2, keepdims=True))
    spread = lax.optimization_barrier(jnp.mean(jnp.square(pre_norm - centre), axis=2, keepdims=True))
    normed = (pre_norm - centre) * lax.rsqrt(spread + norm_eps) * scaling[:, None] + shift_term[:, None]
    return jax.nn.gelu(normed, approximate=False).astype(jnp.bfloat16)

def sample_layers(sample, spectral, skip_weight, skip_bias, norm_gain, norm_shift):
    highest = lax.Precision.HIGHEST
    depth_forward, depth_backward = depth_tables(Z, MZ)
    first_cells = jnp.arange(X, dtype=jnp.int32)
    second_cells = jnp.arange(Y, dtype=jnp.int32)
    second_forward = forward_table(second_cells, signed_freqs(MY), Y, 1.0).astype(jnp.bfloat16)
    first_forward = forward_table(first_cells, signed_freqs(MX), X, 1.0 / math.sqrt(X * Y * Z))
    first_inverse = inverse_table(signed_freqs(MX), first_cells, X).astype(jnp.bfloat16)
    second_inverse = inverse_table(signed_freqs(MY), second_cells, Y)
    inverse_scale = 1.0 / math.sqrt(MX * MY * MZ)
    hidden = sample
    for layer_index in range(LAYERS):
        amplitude = jnp.dot(hidden.reshape(-1, Z).astype(jnp.float32), depth_forward.astype(jnp.float32), precision=highest)
        amplitude = amplitude.astype(jnp.bfloat16).reshape(X, Y, C, 2, MZ)
        along_second = jnp.einsum('xycrz,yrks->xkcsz', amplitude.astype(jnp.float32), second_forward.astype(jnp.float32), precision=highest)
        spectrum_sum = jnp.einsum('xkcsz,xsjt->jkctz', along_second, first_forward, precision=highest)
        spectrum = spectrum_sum.astype(jnp.bfloat16)
        mixed_modes = mix_modes(spectrum.astype(jnp.float32), spectral[layer_index].astype(jnp.float32)).astype(jnp.bfloat16)
        rows_first = jnp.einsum('jkcsz,jsxt->xkctz', mixed_modes.astype(jnp.float32), first_inverse.astype(jnp.float32), precision=highest)
        rows_both = jnp.einsum('xkcsz,ksyt->xyctz', rows_first, second_inverse, precision=highest).astype(jnp.bfloat16)
        spectral_part = jnp.dot(rows_both.reshape(-1, 2 * MZ).astype(jnp.float32), depth_backward.astype(jnp.float32), precision=highest)
        spectral_part = spectral_part.reshape(X, Y, C, Z) * inverse_scale
        skip_part = jnp.einsum('oc,xycz->xyoz', skip_weight[layer_index].astype(jnp.float32), hidden.astype(jnp.float32), precision=highest)
        hidden = finish(spectral_part, skip_part, skip_bias[layer_index], norm_gain[layer_index], norm_shift[layer_index])
    return hidden

def reference(fields, spectral, skip_weight, skip_bias, norm_gain, norm_shift):

    def per_sample(sample):
        return sample_layers(sample, spectral, skip_weight, skip_bias, norm_gain, norm_shift)
    return lax.map(per_sample, fields)
```

```python
import math

import jax
import jax.numpy as jnp
import numpy as np
from jax import lax
from jax.experimental import pallas as pl
from jax.experimental.pallas import tpu as pltpu
from jax.sharding import PartitionSpec as P

X = 128
Y = 128
Z = 128
MX = 16
MY = 16
MZ = 16
C = 32
TX = 8
TY = 32
YH = 4
YL = 8
KB = 4
KL = 4

norm_eps = 1e-05


def signed(count):
    index = np.arange(count)
    return np.where(index < count // 2, index, index - count)


def depth_table():
    phase = 2.0 * np.pi * ((np.arange(Z)[:, None] * np.arange(MZ)[None, :]) % Z) / Z
    parts = np.stack([np.cos(phase), -np.sin(phase)], axis=1)
    full = np.einsum("zrk,ab->azrbk", parts, np.eye(YL))
    return full.reshape(YL * Z, 2 * YL * MZ)


def second_table():
    cells = np.arange(TY)
    phase = 2.0 * np.pi * ((cells[:, None] * signed(MY)[None, :]) % Y) / Y
    cosine, sine = np.cos(phase), np.sin(phase)
    from_real = np.stack([cosine, -sine], axis=-1)
    from_imag = np.stack([sine, cosine], axis=-1)
    both = np.stack([from_real, from_imag], axis=1)
    both = both.reshape(YH, YL, 2, KB, KL, 2)
    full = np.einsum("hlrbkt,vw->hrlvbtkw", both, np.eye(MZ))
    return full.reshape(YH * 2 * YL * MZ, KB * 2 * KL * MZ)


def first_tables():
    cells = np.arange(TX)
    phase = 2.0 * np.pi * ((signed(MX)[:, None] * cells[None, :]) % X) / X
    cosine = np.kron(np.cos(phase), np.eye(C))
    sine = np.kron(np.sin(phase), np.eye(C))
    forward = np.concatenate([cosine, -sine], axis=1)
    backward = np.concatenate([cosine.T, sine.T], axis=0)
    return forward, backward


def turned(value):
    lane = lax.broadcasted_iota(jnp.int32, (1, 128), 1)
    sign = jnp.where(lane < 64, -1.0, 1.0)
    parts = [
        pltpu.roll(value[:, at : at + 128], 64, 1) * sign for at in range(0, value.shape[1], 128)
    ]
    return parts[0] if len(parts) == 1 else jnp.concatenate(parts, axis=1)


def dot(left, right):
    return jnp.dot(left, right, preferred_element_type=jnp.float32)


def dot_nt(left, right):
    return lax.dot_general(
        left, right, (((1,), (1,)), ((), ())), preferred_element_type=jnp.float32
    )


def forward_kernel(fields, depth, second, first, out):
    amplitude = None
    for p in range(YL // 2):
        left = jnp.concatenate(
            [fields[:, :, 2 * p + h].reshape(TX * YH * C, Z) for h in range(2)], axis=1
        )
        term = dot(left, depth[p * 2 * Z : (p + 1) * 2 * Z, :])
        amplitude = term if amplitude is None else amplitude + term
    amplitude = amplitude.astype(jnp.bfloat16).reshape(TX, YH, C, 2 * YL * MZ)
    along = None
    for h in range(YH):
        term = dot(amplitude[:, h].reshape(TX * C, 256), second[h * 256 : (h + 1) * 256, :])
        along = term if along is None else along + term
    both = jnp.concatenate(
        [along.astype(jnp.bfloat16), turned(along).astype(jnp.bfloat16)], axis=0
    )
    modes = dot(first[...], both).astype(jnp.bfloat16)
    for b in range(KB):
        out[:, b] = modes[:, b * 128 : (b + 1) * 128].reshape(MX, C, 128)


def mix_kernel(parts, weight, cosine, sine, spread, out):
    real = jnp.zeros((C, 128), jnp.float32)
    imag = jnp.zeros((C, 128), jnp.float32)
    for s in range(64):
        part = parts[s].astype(jnp.float32)
        real = real + part * cosine[s : s + 1, :]
        imag = imag + part * sine[s : s + 1, :]
    total = (real - turned(imag)) * (1.0 / math.sqrt(X * Y * Z))
    spectrum = dot(spread[...], total.astype(jnp.bfloat16))
    swapped = pltpu.roll(spectrum, 64, 1)
    lane = lax.broadcasted_iota(jnp.int32, (8, 128), 1)
    row = lax.broadcasted_iota(jnp.int32, (8, 128), 0)
    pieces = []
    for b in range(8):
        w = weight[b].astype(jnp.float32)
        same = jnp.sum((spectrum * w).reshape(16, 8, 128), axis=0)
        cross = jnp.sum((swapped * w).reshape(16, 8, 128), axis=0)
        same = same + pltpu.roll(same, 4, 0)
        cross = cross + pltpu.roll(cross, 4, 0)
        same = same - pltpu.roll(same, 64, 1)
        cross = cross + pltpu.roll(cross, 64, 1)
        pieces.append(jnp.where(lane < 64, same, cross))
    mixed = jnp.concatenate(
        [jnp.where(row < 4, pieces[2 * i], pieces[2 * i + 1]) for i in range(4)], axis=0
    )
    mixed_turned = turned(mixed)
    for s in range(64):
        out[s] = (mixed * cosine[s : s + 1, :] + mixed_turned * sine[s : s + 1, :]).astype(
            jnp.bfloat16
        )


def inverse_kernel(
    modes, fields, depth, second, first, skip, bias, gain, shift, out, rows, spectral
):
    h = pl.program_id(0)

    @pl.when(h == 0)
    def _():
        full = jnp.concatenate([modes[:, b].reshape(MX * C, 128) for b in range(KB)], axis=1)
        both = dot(first[...], full)
        lines = both[: TX * C] + turned(both[TX * C :])
        lines = (lines * (1.0 / math.sqrt(MX * MY * MZ))).astype(jnp.bfloat16)
        for i in range(YH):
            rows[i] = dot_nt(lines, second[i * 256 : (i + 1) * 256, :]).astype(jnp.bfloat16)

    spectral[...] = dot_nt(rows[h], depth[...])
    for x in range(0, TX, 2):
        cells = jnp.concatenate(
            [fields[x + i, 0].reshape(YL * C, Z) for i in range(2)], axis=1
        )
        skipped = dot(skip[...], cells)
        for i in range(2):
            for y in range(YL):
                pre = (
                    spectral[(x + i) * C : (x + i + 1) * C, y * Z : (y + 1) * Z]
                    + skipped[y * C : (y + 1) * C, i * Z : (i + 1) * Z]
                    + bias[...]
                )
                centre = jnp.sum(pre, axis=0, keepdims=True) * (1.0 / C)
                pre = pre - centre
                spread = jnp.sum(pre * pre, axis=0, keepdims=True) * (1.0 / C)
                normed = pre * lax.rsqrt(spread + norm_eps) * gain[...] + shift[...]
                half = normed * 0.5
                value = half * lax.erf(normed * math.sqrt(0.5)) + half
                out[x + i, 0, y] = value.astype(jnp.bfloat16)


def local(fields, spectral, skip_weight, skip_bias, norm_gain, norm_shift):
    bf16 = jnp.bfloat16
    hidden = fields.reshape(TX, YH, YL, C, Z)
    depth = jnp.asarray(depth_table(), bf16)
    second = jnp.asarray(second_table(), bf16)
    first_forward, first_backward = first_tables()
    first_forward = jnp.asarray(first_forward, bf16)
    first_backward = jnp.asarray(first_backward, bf16)
    spread = jnp.asarray(np.kron(np.eye(C), np.ones((4, 1))), bf16)

    weight = spectral[0, 0].transpose(2, 3, 1, 0, 4).reshape(128, 128)
    weight = lax.all_to_all(
        jnp.broadcast_to(weight, (8, 128, 128)), "col", split_axis=0, concat_axis=0, tiled=True
    )

    modes = pl.pallas_call(
        forward_kernel,
        out_shape=jax.ShapeDtypeStruct((MX, KB, C, 128), bf16),
        name="forward",
    )(hidden, depth, second, first_forward)
    parts = lax.all_to_all(
        modes.reshape(64, C, 128), ("gx", "gy"), split_axis=0, concat_axis=0, tiled=True
    )

    freq = jnp.arange(16, dtype=jnp.int32)
    freq = jnp.where(freq < 8, freq, freq - 16)
    at_x = lax.axis_index("gx").astype(jnp.int32)
    at_y = lax.axis_index("gy").astype(jnp.int32)
    freq_x = jnp.where(at_x < 8, at_x, at_x - 16)
    lane = lax.broadcasted_iota(jnp.int32, (64, 128), 1)
    place = lax.broadcasted_iota(jnp.int32, (64, 128), 0)
    freq_y = at_y * KL + lane // MZ % KL
    freq_y = jnp.where(freq_y < 8, freq_y, freq_y - 16)
    turn = (freq_x * (place // 4) + freq_y * (place % 4) * 4) % 16
    phase = turn.astype(jnp.float32) * (2.0 * math.pi / 16)
    mixed = pl.pallas_call(
        mix_kernel,
        out_shape=jax.ShapeDtypeStruct((64, C, 128), bf16),
        name="mix",
    )(parts, weight, jnp.cos(phase), jnp.sin(phase), spread)
    full = lax.all_to_all(mixed, ("gx", "gy"), split_axis=0, concat_axis=0, tiled=True)

    skip = jnp.kron(jnp.eye(8, dtype=bf16), skip_weight[0])
    column = lambda v: jnp.broadcast_to(v[0][:, None], (C, Z))
    whole = lambda shape: pl.BlockSpec(shape, lambda h: (0,) * len(shape))
    tile = pl.BlockSpec((TX, 1, YL, C, Z), lambda h: (0, h, 0, 0, 0))
    result = pl.pallas_call(
        inverse_kernel,
        grid=(YH,),
        in_specs=[
            whole((MX, KB, C, 128)),
            tile,
            whole((YL * Z, 256)),
            whole((YH * 256, 512)),
            whole((2 * TX * C, MX * C)),
            whole((256, 256)),
            whole((C, Z)),
            whole((C, Z)),
            whole((C, Z)),
        ],
        out_specs=tile,
        out_shape=jax.ShapeDtypeStruct((TX, YH, YL, C, Z), bf16),
        scratch_shapes=[
            pltpu.VMEM((YH, TX * C, 256), bf16),
            pltpu.VMEM((TX * C, YL * Z), jnp.float32),
        ],
        name="inverse",
    )(
        full.reshape(MX, KB, C, 128),
        hidden,
        depth,
        second,
        first_backward,
        skip,
        column(skip_bias),
        column(norm_gain),
        column(norm_shift),
    )
    return result.reshape(1, TX, TY, C, Z)


def solution(mesh):
    placed = (
        P("col", "gx", "gy", None, None),
        P(None, "gx", "gy", None, None, "col", None),
        P(),
        P(),
        P(),
        P(),
    )
    return jax.shard_map(
        local,
        mesh=mesh,
        in_specs=placed,
        out_specs=P("col", "gx", "gy", None, None),
        check_vma=False,
    )
```

```python
import math

import jax
import jax.numpy as jnp
import numpy as np
from jax import lax
from jax.experimental import pallas as pl
from jax.experimental.pallas import tpu as pltpu
from jax.sharding import PartitionSpec as P


X = 128
Y = 128
Z = 128
MX = 16
MY = 16
MZ = 16
C = 32
TX = 8
TY = 32
YH = 4
YL = 8
KB = 4
KL = 4

norm_eps = 1e-05


def signed(count):
    index = np.arange(count)
    return np.where(index < count // 2, index, index - count)


def depth_table():
    phase = 2.0 * np.pi * ((np.arange(Z)[:, None] * np.arange(MZ)[None, :]) % Z) / Z
    parts = np.stack([np.cos(phase), -np.sin(phase)], axis=1)
    full = np.einsum("zrk,ab->azrbk", parts, np.eye(YL))
    return full.reshape(YL * Z, 2 * YL * MZ)


def second_table():
    cells = np.arange(TY)
    phase = 2.0 * np.pi * ((cells[:, None] * signed(MY)[None, :]) % Y) / Y
    cosine, sine = np.cos(phase), np.sin(phase)
    from_real = np.stack([cosine, -sine], axis=-1)
    from_imag = np.stack([sine, cosine], axis=-1)
    both = np.stack([from_real, from_imag], axis=1)
    both = both.reshape(YH, YL, 2, KB, KL, 2)
    full = np.einsum("hlrbkt,vw->hrlvbtkw", both, np.eye(MZ))
    return full.reshape(YH * 2 * YL * MZ, KB * 2 * KL * MZ)


def first_tables():
    cells = np.arange(TX)
    phase = 2.0 * np.pi * ((signed(MX)[:, None] * cells[None, :]) % X) / X
    cosine = np.kron(np.cos(phase), np.eye(C))
    sine = np.kron(np.sin(phase), np.eye(C))
    forward = np.concatenate([cosine, -sine], axis=1)
    backward = np.concatenate([cosine.T, sine.T], axis=0)
    return forward, backward


def turned(value):
    lane = lax.broadcasted_iota(jnp.int32, (1, 128), 1)
    sign = jnp.where(lane < 64, -1.0, 1.0)
    parts = [
        pltpu.roll(value[:, at : at + 128], 64, 1) * sign for at in range(0, value.shape[1], 128)
    ]
    return parts[0] if len(parts) == 1 else jnp.concatenate(parts, axis=1)


def dot(left, right):
    return jnp.dot(left, right, preferred_element_type=jnp.float32)


def dot_nt(left, right):
    return lax.dot_general(
        left, right, (((1,), (1,)), ((), ())), preferred_element_type=jnp.float32
    )


def forward_kernel(
    fields_far, depth_far, second_far, first_far, out, fields, depth, second, first, sems
):
    half = TX // 2
    pairs = [
        (depth_far, depth),
        (fields_far.at[:half], fields.at[:half]),
        (fields_far.at[half:], fields.at[half:]),
        (second_far, second),
        (first_far, first),
    ]
    copies = [
        pltpu.make_async_copy(here, there, sems.at[n]) for n, (here, there) in enumerate(pairs)
    ]
    for copy in copies:
        copy.start()
    copies[0].wait()
    amplitudes = []
    for part in range(2):
        copies[1 + part].wait()
        amplitude = None
        for p in range(YL // 2):
            left = jnp.concatenate(
                [
                    fields[part * half : (part + 1) * half, :, 2 * p + h].reshape(-1, Z)
                    for h in range(2)
                ],
                axis=1,
            )
            term = dot(left, depth[p * 2 * Z : (p + 1) * 2 * Z, :])
            amplitude = term if amplitude is None else amplitude + term
        amplitudes.append(amplitude.astype(jnp.bfloat16).reshape(half, YH, C, 2 * YL * MZ))
    amplitude = jnp.concatenate(amplitudes, axis=0)
    copies[3].wait()
    along = None
    for h in range(YH):
        term = dot(amplitude[:, h].reshape(TX * C, 256), second[h * 256 : (h + 1) * 256, :])
        along = term if along is None else along + term
    both = jnp.concatenate(
        [along.astype(jnp.bfloat16), turned(along).astype(jnp.bfloat16)], axis=0
    )
    copies[4].wait()
    modes = dot(first[...], both).astype(jnp.bfloat16)
    for b in range(KB):
        for j in range(MX):
            out[j * KB + b] = modes[j * C : (j + 1) * C, b * 128 : (b + 1) * 128]


def prepare_kernel(spectral, out):
    row = lax.broadcasted_iota(jnp.int32, (4 * C, C), 0)
    column = lax.broadcasted_iota(jnp.int32, (4 * C, C), 1)
    total = jnp.zeros((4 * C, 128), jnp.float32)
    for d in range(4):
        piece = jnp.concatenate(
            [spectral[k, r, d] for r in range(2) for k in range(KL)], axis=0
        )
        pick = jnp.where(row == column * 4 + d, 1.0, 0.0).astype(jnp.bfloat16)
        total = total + dot_nt(pick, piece)
    weight = total.astype(jnp.bfloat16)
    for i in range(4):
        out[i] = weight


def position_phases():
    at_x = lax.axis_index("gx").astype(jnp.int32)
    at_y = lax.axis_index("gy").astype(jnp.int32)
    freq_x = jnp.where(at_x < 8, at_x, at_x - 16)
    lane = lax.broadcasted_iota(jnp.int32, (64, 128), 1)
    place = lax.broadcasted_iota(jnp.int32, (64, 128), 0)
    freq_y = at_y * KL + ((lane >> 4) & 3)
    freq_y = jnp.where(freq_y < 8, freq_y, freq_y - 16)
    turn = (freq_x * (place >> 2) + freq_y * (place & 3) * 4) & 15
    cosine = jnp.ones((64, 128), jnp.float32)
    sine = jnp.zeros((64, 128), jnp.float32)
    for n in range(1, 16):
        here = turn == n
        cosine = jnp.where(here, math.cos(2.0 * math.pi * n / 16), cosine)
        sine = jnp.where(here, math.sin(2.0 * math.pi * n / 16), sine)
    return cosine, sine


def collect_kernel(parts, second_far, back_far, out, second, back, cosine, sine, sems):
    copies = [
        pltpu.make_async_copy(second_far, second, sems.at[0]),
        pltpu.make_async_copy(back_far, back, sems.at[1]),
    ]
    for copy in copies:
        copy.start()
    cosine[...], sine[...] = position_phases()
    real = jnp.zeros((C, 128), jnp.float32)
    imag = jnp.zeros((C, 128), jnp.float32)
    for s in range(64):
        part = parts[s].astype(jnp.float32)
        real = real + part * cosine[s : s + 1, :]
        imag = imag + part * sine[s : s + 1, :]
    total = (real - turned(imag)) * (1.0 / math.sqrt(X * Y * Z))
    out[...] = total
    for copy in copies:
        copy.wait()


def mix_kernel(total, near, far, cosine, sine, out):
    row = lax.broadcasted_iota(jnp.int32, (4 * C, C), 0)
    column = lax.broadcasted_iota(jnp.int32, (4 * C, C), 1)
    repeat = jnp.where((row >> 2) == column, 1.0, 0.0).astype(jnp.bfloat16)
    spectrum = dot(repeat, total[...].astype(jnp.bfloat16))
    swapped = pltpu.roll(spectrum, 64, 1)
    lane = lax.broadcasted_iota(jnp.int32, (8, 128), 1)
    row = lax.broadcasted_iota(jnp.int32, (8, 128), 0)

    def mixed_with(weight):
        w = weight.astype(jnp.float32)
        same = jnp.sum((spectrum * w).reshape(16, 8, 128), axis=0)
        cross = jnp.sum((swapped * w).reshape(16, 8, 128), axis=0)
        same = same + pltpu.roll(same, 4, 0)
        cross = cross + pltpu.roll(cross, 4, 0)
        same = same - pltpu.roll(same, 64, 1)
        cross = cross + pltpu.roll(cross, 64, 1)
        return jnp.where(lane < 64, same, cross)

    upper = lax.axis_index("col").astype(jnp.int32) & 1
    nearer = (row >> 2) == upper
    mixed = jnp.concatenate(
        [jnp.where(nearer, mixed_with(near[i]), mixed_with(far[i])) for i in range(4)], axis=0
    )
    mixed_turned = turned(mixed)
    for s in range(64):
        out[s] = (mixed * cosine[s : s + 1, :] + mixed_turned * sine[s : s + 1, :]).astype(
            jnp.bfloat16
        )


def column_of(vector):
    row = lax.broadcasted_iota(jnp.int32, (C, C), 0)
    column = lax.broadcasted_iota(jnp.int32, (C, C), 1)
    spread = jnp.where(row == column, jnp.broadcast_to(vector[...], (C, C)), 0.0)
    return jnp.broadcast_to(jnp.sum(spread, axis=1, keepdims=True), (C, Z))


def inverse_kernel(
    modes, fields, depth, second, first, skip, bias, gain, shift, out, rows, spectral, done, sems
):
    full = jnp.concatenate(
        [
            jnp.concatenate([modes[j * KB + b] for j in range(MX)], axis=0)
            for b in range(KB)
        ],
        axis=1,
    )
    both = dot(first[...], full)
    lines = both[: TX * C] + turned(both[TX * C :])
    lines = (lines * (1.0 / math.sqrt(MX * MY * MZ))).astype(jnp.bfloat16)
    rows[...] = dot_nt(lines, second[...]).astype(jnp.bfloat16)
    row = lax.broadcasted_iota(jnp.int32, (YL * C, YL * C), 0)
    column = lax.broadcasted_iota(jnp.int32, (YL * C, YL * C), 1)
    wide = jnp.concatenate([skip[0]] * YL, axis=1)
    tall = jnp.concatenate([wide] * YL, axis=0).astype(jnp.float32)
    skips = jnp.where((row >> 5) == (column >> 5), tall, 0.0).astype(jnp.bfloat16)
    bias = column_of(bias)
    gain = column_of(gain)
    shift = column_of(shift)
    copies = []
    for h in range(YH):
        spectral[h % 2] = dot_nt(rows[:, h * 256 : (h + 1) * 256], depth[...])
        for x in range(0, TX, 2):
            cells = jnp.concatenate(
                [fields[x + i, h].reshape(YL * C, Z) for i in range(2)], axis=1
            )
            skipped = dot(skips, cells)
            for i in range(2):
                for y in range(YL):
                    pre = (
                        spectral[h % 2, (x + i) * C : (x + i + 1) * C, y * Z : (y + 1) * Z]
                        + skipped[y * C : (y + 1) * C, i * Z : (i + 1) * Z]
                        + bias
                    )
                    centre = jnp.sum(pre, axis=0, keepdims=True) * (1.0 / C)
                    pre = pre - centre
                    spread = jnp.sum(pre * pre, axis=0, keepdims=True) * (1.0 / C)
                    normed = pre * lax.rsqrt(spread + norm_eps) * gain + shift
                    half = normed * 0.5
                    value = half * lax.erf(normed * math.sqrt(0.5)) + half
                    done[h, x + i, y] = value.astype(jnp.bfloat16)
        copy = pltpu.make_async_copy(done.at[h], out.at[:, h], sems.at[h])
        copy.start()
        copies.append(copy)
    for copy in copies:
        copy.wait()


def near(value):
    return pltpu.with_memory_space_constraint(value, pltpu.VMEM)


def far(value):
    return pltpu.with_memory_space_constraint(value, pltpu.HBM)


def local(fields, spectral, skip_weight, skip_bias, norm_gain, norm_shift):
    bf16 = jnp.bfloat16
    hidden = fields.reshape(TX, YH, YL, C, Z)
    depth = jnp.asarray(depth_table(), bf16)
    second = jnp.asarray(second_table(), bf16)
    first_forward, first_backward = first_tables()
    first_forward = jnp.asarray(first_forward, bf16)
    first_backward = jnp.asarray(first_backward, bf16)
    anywhere = pl.BlockSpec(memory_space=pl.ANY)

    weight = pl.pallas_call(
        prepare_kernel,
        out_shape=jax.ShapeDtypeStruct((4, 128, 128), bf16),
        compiler_params=pltpu.CompilerParams(vmem_limit_bytes=8 << 20),
        name="prepare",
    )(spectral[0, 0].transpose(0, 1, 3, 4, 2))
    own = lax.all_to_all(
        weight,
        "col",
        split_axis=0,
        concat_axis=0,
        axis_index_groups=[[0, 2, 4, 6], [1, 3, 5, 7]],
        tiled=True,
    )
    other = lax.ppermute(own, "col", [(i, i ^ 1) for i in range(8)])

    modes, hidden, depth = pl.pallas_call(
        forward_kernel,
        in_specs=[anywhere] * 4,
        out_shape=[
            pltpu.VMEM((64, C, 128), bf16),
            pltpu.VMEM(hidden.shape, bf16),
            pltpu.VMEM(depth.shape, bf16),
        ],
        scratch_shapes=[
            pltpu.VMEM(second.shape, bf16),
            pltpu.VMEM(first_forward.shape, bf16),
            pltpu.SemaphoreType.DMA((5,)),
        ],
        compiler_params=pltpu.CompilerParams(vmem_limit_bytes=20 << 20),
        name="forward",
    )(far(hidden), far(depth), far(second), far(first_forward))
    parts = lax.all_to_all(
        modes, ("gx", "gy"), split_axis=0, concat_axis=0, tiled=True
    )
    inside = pl.BlockSpec(memory_space=pltpu.VMEM)
    total, second, first_backward, cosine, sine = pl.pallas_call(
        collect_kernel,
        in_specs=[inside] + [anywhere] * 2,
        out_shape=[
            pltpu.VMEM((C, 128), jnp.float32),
            pltpu.VMEM(second.shape, bf16),
            pltpu.VMEM(first_backward.shape, bf16),
            pltpu.VMEM((64, 128), jnp.float32),
            pltpu.VMEM((64, 128), jnp.float32),
        ],
        scratch_shapes=[pltpu.SemaphoreType.DMA((2,))],
        compiler_params=pltpu.CompilerParams(vmem_limit_bytes=12 << 20),
        name="collect",
    )(near(parts), far(second), far(first_backward))
    mixed = pl.pallas_call(
        mix_kernel,
        out_shape=pltpu.VMEM((64, C, 128), bf16),
        compiler_params=pltpu.CompilerParams(vmem_limit_bytes=12 << 20),
        name="mix",
    )(total, near(own), near(other), cosine, sine)
    full = lax.all_to_all(mixed, ("gx", "gy"), split_axis=0, concat_axis=0, tiled=True)
    result = pl.pallas_call(
        inverse_kernel,
        out_shape=jax.ShapeDtypeStruct((TX, YH, YL, C, Z), bf16),
        out_specs=anywhere,
        scratch_shapes=[
            pltpu.VMEM((TX * C, YH * 256), bf16),
            pltpu.VMEM((2, TX * C, YL * Z), jnp.float32),
            pltpu.VMEM((YH, TX, YL, C, Z), bf16),
            pltpu.SemaphoreType.DMA((YH,)),
        ],
        compiler_params=pltpu.CompilerParams(vmem_limit_bytes=24 << 20),
        name="inverse",
    )(
        near(full),
        hidden,
        depth,
        second,
        first_backward,
        skip_weight,
        skip_bias,
        norm_gain,
        norm_shift,
    )
    return result.reshape(1, TX, TY, C, Z)


def solution(mesh):
    placed = (
        P("col", "gx", "gy", None, None),
        P(None, "gx", "gy", None, None, "col", None),
        P(),
        P(),
        P(),
        P(),
    )
    return jax.shard_map(
        local,
        mesh=mesh,
        in_specs=placed,
        out_specs=P("col", "gx", "gy", None, None),
        check_vma=False,
    )
```

```python
import math

import jax
import jax.numpy as jnp
import numpy as np
from jax import lax
from jax.experimental import pallas as pl
from jax.experimental.pallas import tpu as pltpu
from jax.sharding import PartitionSpec as P


X = 128
Y = 128
Z = 128
MX = 16
MY = 16
MZ = 16
C = 32
TX = 8
TY = 32
YH = 4
YL = 8
KB = 4
KL = 4

norm_eps = 1e-05


def signed(count):
    index = np.arange(count)
    return np.where(index < count // 2, index, index - count)


def depth_table():
    phase = 2.0 * np.pi * ((np.arange(Z)[:, None] * np.arange(MZ)[None, :]) % Z) / Z
    parts = np.stack([np.cos(phase), -np.sin(phase)], axis=1)
    full = np.einsum("zrk,ab->azrbk", parts, np.eye(YL))
    return full.reshape(YL * Z, 2 * YL * MZ)


def second_table():
    cells = np.arange(TY)
    phase = 2.0 * np.pi * ((cells[:, None] * signed(MY)[None, :]) % Y) / Y
    cosine, sine = np.cos(phase), np.sin(phase)
    from_real = np.stack([cosine, -sine], axis=-1)
    from_imag = np.stack([sine, cosine], axis=-1)
    both = np.stack([from_real, from_imag], axis=1)
    both = both.reshape(YH, YL, 2, KB, KL, 2)
    full = np.einsum("hlrbkt,vw->hrlvbtkw", both, np.eye(MZ))
    return full.reshape(YH * 2 * YL * MZ, KB * 2 * KL * MZ)


def first_tables():
    cells = np.arange(TX)
    phase = 2.0 * np.pi * ((signed(MX)[:, None] * cells[None, :]) % X) / X
    cosine = np.kron(np.cos(phase), np.eye(C))
    sine = np.kron(np.sin(phase), np.eye(C))
    forward = np.concatenate([cosine, -sine], axis=1)
    backward = np.concatenate([cosine.T, sine.T], axis=0)
    return forward, backward


def turned(value):
    lane = lax.broadcasted_iota(jnp.int32, (1, 128), 1)
    sign = jnp.where(lane < 64, -1.0, 1.0)
    parts = [
        pltpu.roll(value[:, at : at + 128], 64, 1) * sign for at in range(0, value.shape[1], 128)
    ]
    return parts[0] if len(parts) == 1 else jnp.concatenate(parts, axis=1)


def dot(left, right):
    return jnp.dot(left, right, preferred_element_type=jnp.float32)


def dot_nt(left, right):
    return lax.dot_general(
        left, right, (((1,), (1,)), ((), ())), preferred_element_type=jnp.float32
    )


def forward_kernel(
    fields_far, depth_far, second_far, first_far, out_far, fields, depth, second, first, out, sems
):
    half = TX // 2
    pairs = [
        (depth_far, depth),
        (fields_far.at[:half], fields.at[:half]),
        (fields_far.at[half:], fields.at[half:]),
        (second_far, second),
        (first_far, first),
    ]
    copies = [
        pltpu.make_async_copy(here, there, sems.at[n]) for n, (here, there) in enumerate(pairs)
    ]
    for copy in copies[:3]:
        copy.start()
    copies[0].wait()
    amplitudes = []
    for part in range(2):
        copies[1 + part].wait()
        copies[3 + part].start()
        amplitude = None
        for p in range(YL // 2):
            left = jnp.concatenate(
                [
                    fields[part * half : (part + 1) * half, :, 2 * p + h].reshape(-1, Z)
                    for h in range(2)
                ],
                axis=1,
            )
            term = dot(left, depth[p * 2 * Z : (p + 1) * 2 * Z, :])
            amplitude = term if amplitude is None else amplitude + term
        amplitudes.append(amplitude.astype(jnp.bfloat16).reshape(half, YH, C, 2 * YL * MZ))
    amplitude = jnp.concatenate(amplitudes, axis=0)
    copies[3].wait()
    along = None
    for h in range(YH):
        term = dot(amplitude[:, h].reshape(TX * C, 256), second[h * 256 : (h + 1) * 256, :])
        along = term if along is None else along + term
    both = jnp.concatenate(
        [along.astype(jnp.bfloat16), turned(along).astype(jnp.bfloat16)], axis=0
    )
    copies[4].wait()
    sent = []
    for g in range(4):
        modes = dot(first[g * 4 * C : (g + 1) * 4 * C, :], both).astype(jnp.bfloat16)
        for b in range(KB):
            for j in range(4):
                out[(g * 4 + j) * KB + b] = modes[j * C : (j + 1) * C, b * 128 : (b + 1) * 128]
        copy = pltpu.make_async_copy(
            out.at[g * 16 : (g + 1) * 16], out_far.at[g * 16 : (g + 1) * 16], sems.at[5 + g]
        )
        copy.start()
        sent.append(copy)
    for copy in sent:
        copy.wait()


def prepare_kernel(own, other, out):
    row = lax.broadcasted_iota(jnp.int32, (4 * C, C), 0)
    column = lax.broadcasted_iota(jnp.int32, (4 * C, C), 1)
    for n, source in enumerate((own, other)):
        total = jnp.zeros((4 * C, 128), jnp.float32)
        for d in range(4):
            piece = jnp.concatenate(
                [source[k, r, d] for r in range(2) for k in range(KL)], axis=0
            )
            pick = jnp.where(row == column * 4 + d, 1.0, 0.0).astype(jnp.bfloat16)
            total = total + dot_nt(pick, piece)
        out[n] = total.astype(jnp.bfloat16)


def position_phases():
    at_x = lax.axis_index("gx").astype(jnp.int32)
    at_y = lax.axis_index("gy").astype(jnp.int32)
    freq_x = jnp.where(at_x < 8, at_x, at_x - 16)
    lane = lax.broadcasted_iota(jnp.int32, (64, 128), 1)
    place = lax.broadcasted_iota(jnp.int32, (64, 128), 0)
    freq_y = at_y * KL + ((lane >> 4) & 3)
    freq_y = jnp.where(freq_y < 8, freq_y, freq_y - 16)
    turn = (freq_x * (place >> 2) + freq_y * (place & 3) * 4) & 15
    cosine = jnp.ones((64, 128), jnp.float32)
    sine = jnp.zeros((64, 128), jnp.float32)
    for n in range(1, 16):
        here = turn == n
        cosine = jnp.where(here, math.cos(2.0 * math.pi * n / 16), cosine)
        sine = jnp.where(here, math.sin(2.0 * math.pi * n / 16), sine)
    return cosine, sine


def collect_kernel(parts, out, cosine, sine):
    cosine[...], sine[...] = position_phases()
    real = jnp.zeros((C, 128), jnp.float32)
    imag = jnp.zeros((C, 128), jnp.float32)
    for s in range(64):
        part = parts[s].astype(jnp.float32)
        real = real + part * cosine[s : s + 1, :]
        imag = imag + part * sine[s : s + 1, :]
    total = (real - turned(imag)) * (1.0 / math.sqrt(X * Y * Z))
    out[...] = total


def mix_kernel(total, here, before, after, across, cosine, sine, out):
    row = lax.broadcasted_iota(jnp.int32, (4 * C, C), 0)
    column = lax.broadcasted_iota(jnp.int32, (4 * C, C), 1)
    repeat = jnp.where((row >> 2) == column, 1.0, 0.0).astype(jnp.bfloat16)
    spectrum = dot(repeat, total[...].astype(jnp.bfloat16))
    swapped = pltpu.roll(spectrum, 64, 1)
    lane = lax.broadcasted_iota(jnp.int32, (8, 128), 1)
    row = lax.broadcasted_iota(jnp.int32, (8, 128), 0)

    def mixed_with(weight):
        w = weight.astype(jnp.float32)
        same = jnp.sum((spectrum * w).reshape(16, 8, 128), axis=0)
        cross = jnp.sum((swapped * w).reshape(16, 8, 128), axis=0)
        same = same + pltpu.roll(same, 4, 0)
        cross = cross + pltpu.roll(cross, 4, 0)
        same = same - pltpu.roll(same, 64, 1)
        cross = cross + pltpu.roll(cross, 64, 1)
        return jnp.where(lane < 64, same, cross)

    place = lax.axis_index("col").astype(jnp.int32)
    nearer = (row >> 2) == (place & 1)
    blocks = [jnp.zeros((8, 128), jnp.float32) for _ in range(4)]
    for offset, weight in ((0, here), (3, before), (1, after), (2, across)):
        block = jnp.where(nearer, mixed_with(weight[0]), mixed_with(weight[1]))
        source = ((place >> 1) + offset) & 3
        blocks = [jnp.where(source == i, block, blocks[i]) for i in range(4)]
    mixed = jnp.concatenate(blocks, axis=0)
    mixed_turned = turned(mixed)
    for s in range(64):
        out[s] = (mixed * cosine[s : s + 1, :] + mixed_turned * sine[s : s + 1, :]).astype(
            jnp.bfloat16
        )


def column_of(vector):
    row = lax.broadcasted_iota(jnp.int32, (C, C), 0)
    column = lax.broadcasted_iota(jnp.int32, (C, C), 1)
    spread = jnp.where(row == column, jnp.broadcast_to(vector[...], (C, C)), 0.0)
    return jnp.broadcast_to(jnp.sum(spread, axis=1, keepdims=True), (C, Z))


def inverse_kernel(
    modes, fields, depth, second, first, skip, bias, gain, shift, out, rows, spectral, done, sems
):
    full = jnp.concatenate(
        [
            jnp.concatenate([modes[j * KB + b] for j in range(MX)], axis=0)
            for b in range(KB)
        ],
        axis=1,
    )
    both = dot(first[...], full)
    lines = both[: TX * C] + turned(both[TX * C :])
    lines = (lines * (1.0 / math.sqrt(MX * MY * MZ))).astype(jnp.bfloat16)
    rows[...] = dot_nt(lines, second[...]).astype(jnp.bfloat16)
    row = lax.broadcasted_iota(jnp.int32, (YL * C, YL * C), 0)
    column = lax.broadcasted_iota(jnp.int32, (YL * C, YL * C), 1)
    wide = jnp.concatenate([skip[0]] * YL, axis=1)
    tall = jnp.concatenate([wide] * YL, axis=0).astype(jnp.float32)
    skips = jnp.where((row >> 5) == (column >> 5), tall, 0.0).astype(jnp.bfloat16)
    bias = column_of(bias)
    gain = column_of(gain)
    shift = column_of(shift)
    copies = []
    for h in range(YH):
        spectral[h % 2] = dot_nt(rows[:, h * 256 : (h + 1) * 256], depth[...])
        for x in range(0, TX, 2):
            cells = jnp.concatenate(
                [fields[x + i, h].reshape(YL * C, Z) for i in range(2)], axis=1
            )
            skipped = dot(skips, cells)
            for i in range(2):
                for y in range(YL):
                    pre = (
                        spectral[h % 2, (x + i) * C : (x + i + 1) * C, y * Z : (y + 1) * Z]
                        + skipped[y * C : (y + 1) * C, i * Z : (i + 1) * Z]
                        + bias
                    )
                    centre = jnp.sum(pre, axis=0, keepdims=True) * (1.0 / C)
                    pre = pre - centre
                    spread = jnp.sum(pre * pre, axis=0, keepdims=True) * (1.0 / C)
                    normed = pre * lax.rsqrt(spread + norm_eps) * gain + shift
                    half = normed * 0.5
                    value = half * lax.erf(normed * math.sqrt(0.5)) + half
                    done[h, x + i, y] = value.astype(jnp.bfloat16)
        copy = pltpu.make_async_copy(done.at[h], out.at[:, h], sems.at[h])
        copy.start()
        copies.append(copy)
    for copy in copies:
        copy.wait()


def near(value):
    return pltpu.with_memory_space_constraint(value, pltpu.VMEM)


def far(value):
    return pltpu.with_memory_space_constraint(value, pltpu.HBM)


def local(fields, spectral, skip_weight, skip_bias, norm_gain, norm_shift):
    bf16 = jnp.bfloat16
    hidden = fields.reshape(TX, YH, YL, C, Z)
    depth = jnp.asarray(depth_table(), bf16)
    second = jnp.asarray(second_table(), bf16)
    first_forward, first_backward = first_tables()
    first_forward = jnp.asarray(first_forward, bf16)
    first_backward = jnp.asarray(first_backward, bf16)
    anywhere = pl.BlockSpec(memory_space=pl.ANY)

    raw = spectral[0, 0].transpose(0, 1, 3, 4, 2)
    partner = lax.ppermute(raw, "col", [(i, i ^ 1) for i in range(8)])
    weight = pl.pallas_call(
        prepare_kernel,
        out_shape=jax.ShapeDtypeStruct((2, 128, 128), bf16),
        compiler_params=pltpu.CompilerParams(vmem_limit_bytes=8 << 20),
        name="prepare",
    )(raw, partner)
    around = []
    for step in (2, 6, 4):
        around.append(
            lax.ppermute(weight, "col", [(i, (i + step) % 8) for i in range(8)])
        )

    modes, hidden = pl.pallas_call(
        forward_kernel,
        in_specs=[anywhere] * 4,
        out_shape=[
            pltpu.HBM((64, C, 128), bf16),
            pltpu.VMEM(hidden.shape, bf16),
        ],
        scratch_shapes=[
            pltpu.VMEM(depth.shape, bf16),
            pltpu.VMEM(second.shape, bf16),
            pltpu.VMEM(first_forward.shape, bf16),
            pltpu.VMEM((64, C, 128), bf16),
            pltpu.SemaphoreType.DMA((9,)),
        ],
        compiler_params=pltpu.CompilerParams(vmem_limit_bytes=20 << 20),
        name="forward",
    )(far(hidden), far(depth), far(second), far(first_forward))
    parts = lax.all_to_all(
        modes, ("gx", "gy"), split_axis=0, concat_axis=0, tiled=True
    )
    total, cosine, sine = pl.pallas_call(
        collect_kernel,
        out_shape=[
            pltpu.VMEM((C, 128), jnp.float32),
            pltpu.VMEM((64, 128), jnp.float32),
            pltpu.VMEM((64, 128), jnp.float32),
        ],
        compiler_params=pltpu.CompilerParams(vmem_limit_bytes=12 << 20),
        name="collect",
    )(near(parts))
    mixed = pl.pallas_call(
        mix_kernel,
        out_shape=pltpu.VMEM((64, C, 128), bf16),
        compiler_params=pltpu.CompilerParams(vmem_limit_bytes=12 << 20),
        name="mix",
    )(total, near(weight), *[near(w) for w in around], cosine, sine)
    full = lax.all_to_all(mixed, ("gx", "gy"), split_axis=0, concat_axis=0, tiled=True)
    result = pl.pallas_call(
        inverse_kernel,
        out_shape=jax.ShapeDtypeStruct((TX, YH, YL, C, Z), bf16),
        out_specs=anywhere,
        scratch_shapes=[
            pltpu.VMEM((TX * C, YH * 256), bf16),
            pltpu.VMEM((2, TX * C, YL * Z), jnp.float32),
            pltpu.VMEM((YH, TX, YL, C, Z), bf16),
            pltpu.SemaphoreType.DMA((YH,)),
        ],
        compiler_params=pltpu.CompilerParams(vmem_limit_bytes=24 << 20),
        name="inverse",
    )(
        near(full),
        hidden,
        near(depth),
        near(second),
        near(first_backward),
        skip_weight,
        skip_bias,
        norm_gain,
        norm_shift,
    )
    return result.reshape(1, TX, TY, C, Z)


def solution(mesh):
    placed = (
        P("col", "gx", "gy", None, None),
        P(None, "gx", "gy", None, None, "col", None),
        P(),
        P(),
        P(),
        P(),
    )
    return jax.shard_map(
        local,
        mesh=mesh,
        in_specs=placed,
        out_specs=P("col", "gx", "gy", None, None),
        check_vma=False,
    )
```

```python
import math

import jax
import jax.numpy as jnp
import numpy as np
from jax import lax
from jax.experimental import pallas as pl
from jax.experimental.pallas import tpu as pltpu
from jax.sharding import PartitionSpec as P


X = 128
Y = 128
Z = 128
MX = 16
MY = 16
MZ = 16
C = 32
TX = 8
TY = 32
YH = 4
YL = 8
KB = 4
KL = 4

norm_eps = 1e-05


def signed(count):
    index = np.arange(count)
    return np.where(index < count // 2, index, index - count)


def depth_table():
    phase = 2.0 * np.pi * ((np.arange(Z)[:, None] * np.arange(MZ)[None, :]) % Z) / Z
    parts = np.stack([np.cos(phase), -np.sin(phase)], axis=1)
    full = np.einsum("zrk,ab->azrbk", parts, np.eye(YL))
    return full.reshape(YL * Z, 2 * YL * MZ)


def second_table():
    cells = np.arange(TY)
    phase = 2.0 * np.pi * ((cells[:, None] * signed(MY)[None, :]) % Y) / Y
    cosine, sine = np.cos(phase), np.sin(phase)
    from_real = np.stack([cosine, -sine], axis=-1)
    from_imag = np.stack([sine, cosine], axis=-1)
    both = np.stack([from_real, from_imag], axis=1)
    both = both.reshape(YH, YL, 2, KB, KL, 2)
    full = np.einsum("hlrbkt,vw->hrlvbtkw", both, np.eye(MZ))
    return full.reshape(YH * 2 * YL * MZ, KB * 2 * KL * MZ)


def first_tables():
    cells = np.arange(TX)
    phase = 2.0 * np.pi * ((signed(MX)[:, None] * cells[None, :]) % X) / X
    cosine = np.kron(np.cos(phase), np.eye(C))
    sine = np.kron(np.sin(phase), np.eye(C))
    forward = np.concatenate([cosine, -sine], axis=1)
    backward = np.concatenate([cosine.T, sine.T], axis=0)
    return forward, backward


def turned(value):
    lane = lax.broadcasted_iota(jnp.int32, (1, 128), 1)
    sign = jnp.where(lane < 64, -1.0, 1.0)
    parts = [
        pltpu.roll(value[:, at : at + 128], 64, 1) * sign for at in range(0, value.shape[1], 128)
    ]
    return parts[0] if len(parts) == 1 else jnp.concatenate(parts, axis=1)


def dot(left, right):
    return jnp.dot(left, right, preferred_element_type=jnp.float32)


def dot_nt(left, right):
    return lax.dot_general(
        left, right, (((1,), (1,)), ((), ())), preferred_element_type=jnp.float32
    )


def forward_kernel(
    fields_far, depth_far, second_far, first_far, out_far, fields, depth, second, first, out, sems
):
    half = TX // 2
    pairs = [
        (depth_far, depth),
        (fields_far.at[:half], fields.at[:half]),
        (fields_far.at[half:], fields.at[half:]),
        (second_far, second),
        (first_far, first),
    ]
    copies = [
        pltpu.make_async_copy(here, there, sems.at[n]) for n, (here, there) in enumerate(pairs)
    ]
    for copy in copies:
        copy.start()
    copies[0].wait()
    amplitudes = []
    for part in range(2):
        copies[1 + part].wait()
        amplitude = None
        for p in range(YL // 2):
            left = jnp.concatenate(
                [
                    fields[part * half : (part + 1) * half, :, 2 * p + h].reshape(-1, Z)
                    for h in range(2)
                ],
                axis=1,
            )
            term = dot(left, depth[p * 2 * Z : (p + 1) * 2 * Z, :])
            amplitude = term if amplitude is None else amplitude + term
        amplitudes.append(amplitude.astype(jnp.bfloat16).reshape(half, YH, C, 2 * YL * MZ))
    amplitude = jnp.concatenate(amplitudes, axis=0)
    copies[3].wait()
    along = None
    for h in range(YH):
        term = dot(amplitude[:, h].reshape(TX * C, 256), second[h * 256 : (h + 1) * 256, :])
        along = term if along is None else along + term
    both = jnp.concatenate(
        [along.astype(jnp.bfloat16), turned(along).astype(jnp.bfloat16)], axis=0
    )
    copies[4].wait()
    sent = []
    for g in range(4):
        modes = dot(first[g * 4 * C : (g + 1) * 4 * C, :], both).astype(jnp.bfloat16)
        for b in range(KB):
            for j in range(4):
                out[(g * 4 + j) * KB + b] = modes[j * C : (j + 1) * C, b * 128 : (b + 1) * 128]
        copy = pltpu.make_async_copy(
            out.at[g * 16 : (g + 1) * 16], out_far.at[g * 16 : (g + 1) * 16], sems.at[5 + g]
        )
        copy.start()
        sent.append(copy)
    for copy in sent:
        copy.wait()


def prepare_kernel(own, other, out):
    row = lax.broadcasted_iota(jnp.int32, (4 * C, C), 0)
    column = lax.broadcasted_iota(jnp.int32, (4 * C, C), 1)
    for n, source in enumerate((own, other)):
        total = jnp.zeros((4 * C, 128), jnp.float32)
        for d in range(4):
            piece = jnp.concatenate(
                [source[k, r, d] for r in range(2) for k in range(KL)], axis=0
            )
            pick = jnp.where(row == column * 4 + d, 1.0, 0.0).astype(jnp.bfloat16)
            total = total + dot_nt(pick, piece)
        out[n] = total.astype(jnp.bfloat16)


def position_phases():
    at_x = lax.axis_index("gx").astype(jnp.int32)
    at_y = lax.axis_index("gy").astype(jnp.int32)
    freq_x = jnp.where(at_x < 8, at_x, at_x - 16)
    lane = lax.broadcasted_iota(jnp.int32, (64, 128), 1)
    place = lax.broadcasted_iota(jnp.int32, (64, 128), 0)
    freq_y = at_y * KL + ((lane >> 4) & 3)
    freq_y = jnp.where(freq_y < 8, freq_y, freq_y - 16)
    turn = (freq_x * (place >> 2) + freq_y * (place & 3) * 4) & 15
    cosine = jnp.ones((64, 128), jnp.float32)
    sine = jnp.zeros((64, 128), jnp.float32)
    for n in range(1, 16):
        here = turn == n
        cosine = jnp.where(here, math.cos(2.0 * math.pi * n / 16), cosine)
        sine = jnp.where(here, math.sin(2.0 * math.pi * n / 16), sine)
    return cosine, sine


def collect_kernel(parts_far, out, cosine, sine, parts, sems):
    copies = [
        pltpu.make_async_copy(
            parts_far.at[g * 16 : (g + 1) * 16], parts.at[g * 16 : (g + 1) * 16], sems.at[g]
        )
        for g in range(4)
    ]
    for copy in copies:
        copy.start()
    cosine[...], sine[...] = position_phases()
    real = jnp.zeros((C, 128), jnp.float32)
    imag = jnp.zeros((C, 128), jnp.float32)
    for s in range(64):
        if s % 16 == 0:
            copies[s // 16].wait()
        part = parts[s].astype(jnp.float32)
        real = real + part * cosine[s : s + 1, :]
        imag = imag + part * sine[s : s + 1, :]
    total = (real - turned(imag)) * (1.0 / math.sqrt(X * Y * Z))
    out[...] = total


def mix_kernel(total, here, before, after, across, cosine, sine, out):
    row = lax.broadcasted_iota(jnp.int32, (4 * C, C), 0)
    column = lax.broadcasted_iota(jnp.int32, (4 * C, C), 1)
    repeat = jnp.where((row >> 2) == column, 1.0, 0.0).astype(jnp.bfloat16)
    spectrum = dot(repeat, total[...].astype(jnp.bfloat16))
    swapped = pltpu.roll(spectrum, 64, 1)
    lane = lax.broadcasted_iota(jnp.int32, (8, 128), 1)
    row = lax.broadcasted_iota(jnp.int32, (8, 128), 0)

    def mixed_with(weight):
        w = weight.astype(jnp.float32)
        same = jnp.sum((spectrum * w).reshape(16, 8, 128), axis=0)
        cross = jnp.sum((swapped * w).reshape(16, 8, 128), axis=0)
        same = same + pltpu.roll(same, 4, 0)
        cross = cross + pltpu.roll(cross, 4, 0)
        same = same - pltpu.roll(same, 64, 1)
        cross = cross + pltpu.roll(cross, 64, 1)
        return jnp.where(lane < 64, same, cross)

    place = lax.axis_index("col").astype(jnp.int32)
    nearer = (row >> 2) == (place & 1)
    blocks = [jnp.zeros((8, 128), jnp.float32) for _ in range(4)]
    for offset, weight in ((0, here), (3, before), (1, after), (2, across)):
        block = jnp.where(nearer, mixed_with(weight[0]), mixed_with(weight[1]))
        source = ((place >> 1) + offset) & 3
        blocks = [jnp.where(source == i, block, blocks[i]) for i in range(4)]
    mixed = jnp.concatenate(blocks, axis=0)
    mixed_turned = turned(mixed)
    for s in range(64):
        out[s] = (mixed * cosine[s : s + 1, :] + mixed_turned * sine[s : s + 1, :]).astype(
            jnp.bfloat16
        )


def column_of(vector):
    row = lax.broadcasted_iota(jnp.int32, (C, C), 0)
    column = lax.broadcasted_iota(jnp.int32, (C, C), 1)
    spread = jnp.where(row == column, jnp.broadcast_to(vector[...], (C, C)), 0.0)
    return jnp.broadcast_to(jnp.sum(spread, axis=1, keepdims=True), (C, Z))


def inverse_kernel(
    modes, fields, depth, second, first, skip, bias, gain, shift, out, rows, spectral, done, sems
):
    full = jnp.concatenate(
        [
            jnp.concatenate([modes[j * KB + b] for j in range(MX)], axis=0)
            for b in range(KB)
        ],
        axis=1,
    )
    both = dot(first[...], full)
    lines = both[: TX * C] + turned(both[TX * C :])
    lines = lines * (1.0 / math.sqrt(MX * MY * MZ))
    lines = lines.reshape(TX, C, YH * 128)
    lines = lines - jnp.sum(lines, axis=1, keepdims=True) * (1.0 / C)
    lines = lines.reshape(TX * C, YH * 128).astype(jnp.bfloat16)
    rows[...] = dot_nt(lines, second[...]).astype(jnp.bfloat16)
    row = lax.broadcasted_iota(jnp.int32, (YL * C, YL * C), 0)
    column = lax.broadcasted_iota(jnp.int32, (YL * C, YL * C), 1)
    block = (row >> 5) == (column >> 5)
    square = skip[0].astype(jnp.float32)
    square = square - jnp.sum(square, axis=0, keepdims=True) * (1.0 / C)
    wide = jnp.concatenate([square] * YL, axis=1)
    tall = jnp.where(block, jnp.concatenate([wide] * YL, axis=0), 0.0)
    coarse = tall.astype(jnp.bfloat16)
    fine = (tall - coarse.astype(jnp.float32)).astype(jnp.bfloat16)
    bias = column_of(bias)
    bias = bias - jnp.sum(bias, axis=0, keepdims=True) * (1.0 / C)
    gain = column_of(gain) * math.sqrt(0.5)
    shift = column_of(shift) * math.sqrt(0.5)
    copies = []
    for h in range(YH):
        spectral[h % 2] = dot_nt(rows[:, h * 256 : (h + 1) * 256], depth[...])
        for x in range(0, TX, 2):
            cells = jnp.concatenate(
                [fields[x + i, h].reshape(YL * C, Z) for i in range(2)], axis=1
            )
            skipped = dot(coarse, cells) + dot(fine, cells)
            for i in range(2):
                for y in range(YL):
                    pre = (
                        spectral[h % 2, (x + i) * C : (x + i + 1) * C, y * Z : (y + 1) * Z]
                        + skipped[y * C : (y + 1) * C, i * Z : (i + 1) * Z]
                        + bias
                    )
                    spread = jnp.sum(pre * pre, axis=0, keepdims=True) * (1.0 / C)
                    normed = pre * lax.rsqrt(spread + norm_eps) * gain + shift
                    half = normed * math.sqrt(0.5)
                    done[h, x + i, y] = (half * lax.erf(normed) + half).astype(jnp.bfloat16)
            copy = pltpu.make_async_copy(
                done.at[h, x : x + 2], out.at[x : x + 2, h], sems.at[h * 4 + x // 2]
            )
            copy.start()
            copies.append(copy)
    for copy in copies:
        copy.wait()


def near(value):
    return pltpu.with_memory_space_constraint(value, pltpu.VMEM)


def far(value):
    return pltpu.with_memory_space_constraint(value, pltpu.HBM)


def local(fields, spectral, skip_weight, skip_bias, norm_gain, norm_shift):
    bf16 = jnp.bfloat16
    hidden = fields.reshape(TX, YH, YL, C, Z)
    depth = jnp.asarray(depth_table(), bf16)
    second = jnp.asarray(second_table(), bf16)
    first_forward, first_backward = first_tables()
    first_forward = jnp.asarray(first_forward, bf16)
    first_backward = jnp.asarray(first_backward, bf16)
    anywhere = pl.BlockSpec(memory_space=pl.ANY)

    raw = spectral[0, 0].transpose(0, 1, 3, 4, 2)
    partner = lax.ppermute(raw, "col", [(i, i ^ 1) for i in range(8)])
    weight = pl.pallas_call(
        prepare_kernel,
        out_shape=jax.ShapeDtypeStruct((2, 128, 128), bf16),
        compiler_params=pltpu.CompilerParams(vmem_limit_bytes=8 << 20),
        name="prepare",
    )(raw, partner)
    around = []
    for step in (2, 6, 4):
        around.append(
            lax.ppermute(weight, "col", [(i, (i + step) % 8) for i in range(8)])
        )

    modes, hidden = pl.pallas_call(
        forward_kernel,
        in_specs=[anywhere] * 4,
        out_shape=[
            pltpu.HBM((64, C, 128), bf16),
            pltpu.VMEM(hidden.shape, bf16),
        ],
        scratch_shapes=[
            pltpu.VMEM(depth.shape, bf16),
            pltpu.VMEM(second.shape, bf16),
            pltpu.VMEM(first_forward.shape, bf16),
            pltpu.VMEM((64, C, 128), bf16),
            pltpu.SemaphoreType.DMA((9,)),
        ],
        compiler_params=pltpu.CompilerParams(vmem_limit_bytes=20 << 20),
        name="forward",
    )(far(hidden), far(depth), far(second), far(first_forward))
    parts = lax.all_to_all(
        modes, ("gx", "gy"), split_axis=0, concat_axis=0, tiled=True
    )
    total, cosine, sine = pl.pallas_call(
        collect_kernel,
        in_specs=[anywhere],
        scratch_shapes=[pltpu.VMEM((64, C, 128), bf16), pltpu.SemaphoreType.DMA((4,))],
        out_shape=[
            pltpu.VMEM((C, 128), jnp.float32),
            pltpu.VMEM((64, 128), jnp.float32),
            pltpu.VMEM((64, 128), jnp.float32),
        ],
        compiler_params=pltpu.CompilerParams(vmem_limit_bytes=12 << 20),
        name="collect",
    )(far(parts))
    mixed = pl.pallas_call(
        mix_kernel,
        out_shape=pltpu.VMEM((64, C, 128), bf16),
        compiler_params=pltpu.CompilerParams(vmem_limit_bytes=12 << 20),
        name="mix",
    )(total, near(weight), *[near(w) for w in around], cosine, sine)
    full = lax.all_to_all(mixed, ("gx", "gy"), split_axis=0, concat_axis=0, tiled=True)
    result = pl.pallas_call(
        inverse_kernel,
        out_shape=jax.ShapeDtypeStruct((TX, YH, YL, C, Z), bf16),
        out_specs=anywhere,
        scratch_shapes=[
            pltpu.VMEM((TX * C, YH * 256), bf16),
            pltpu.VMEM((2, TX * C, YL * Z), jnp.float32),
            pltpu.VMEM((YH, TX, YL, C, Z), bf16),
            pltpu.SemaphoreType.DMA((YH * 4,)),
        ],
        compiler_params=pltpu.CompilerParams(vmem_limit_bytes=24 << 20),
        name="inverse",
    )(
        near(full),
        hidden,
        near(depth),
        near(second),
        near(first_backward),
        skip_weight,
        skip_bias,
        norm_gain,
        norm_shift,
    )
    return result.reshape(1, TX, TY, C, Z)


def solution(mesh):
    placed = (
        P("col", "gx", "gy", None, None),
        P(None, "gx", "gy", None, None, "col", None),
        P(),
        P(),
        P(),
        P(),
    )
    return jax.shard_map(
        local,
        mesh=mesh,
        in_specs=placed,
        out_specs=P("col", "gx", "gy", None, None),
        check_vma=False,
    )
```

```python
import math

import jax
import jax.numpy as jnp
import numpy as np
from jax import lax
from jax.experimental import pallas as pl
from jax.experimental.pallas import tpu as pltpu
from jax.sharding import PartitionSpec as P


X = 128
Y = 128
Z = 128
MX = 16
MY = 16
MZ = 16
C = 32
TX = 8
TY = 32
YH = 4
YL = 8
KB = 4
KL = 4

norm_eps = 1e-05


def signed(count):
    index = np.arange(count)
    return np.where(index < count // 2, index, index - count)


def depth_table():
    phase = 2.0 * np.pi * ((np.arange(Z)[:, None] * np.arange(MZ)[None, :]) % Z) / Z
    parts = np.stack([np.cos(phase), -np.sin(phase)], axis=1)
    full = np.einsum("zrk,ab->azrbk", parts, np.eye(YL))
    return full.reshape(YL * Z, 2 * YL * MZ)


def second_table():
    cells = np.arange(TY)
    phase = 2.0 * np.pi * ((cells[:, None] * signed(MY)[None, :]) % Y) / Y
    cosine, sine = np.cos(phase), np.sin(phase)
    from_real = np.stack([cosine, -sine], axis=-1)
    from_imag = np.stack([sine, cosine], axis=-1)
    both = np.stack([from_real, from_imag], axis=1)
    both = both.reshape(YH, YL, 2, KB, KL, 2)
    full = np.einsum("hlrbkt,vw->hrlvbtkw", both, np.eye(MZ))
    return full.reshape(YH * 2 * YL * MZ, KB * 2 * KL * MZ)


def first_tables():
    cells = np.arange(TX)
    phase = 2.0 * np.pi * ((signed(MX)[:, None] * cells[None, :]) % X) / X
    cosine = np.kron(np.cos(phase), np.eye(C))
    sine = np.kron(np.sin(phase), np.eye(C))
    forward = np.concatenate([cosine, -sine], axis=1)
    backward = np.concatenate([cosine.T, sine.T], axis=0)
    return forward, backward


def turned(value):
    lane = lax.broadcasted_iota(jnp.int32, (1, 128), 1)
    sign = jnp.where(lane < 64, -1.0, 1.0)
    parts = [
        pltpu.roll(value[:, at : at + 128], 64, 1) * sign for at in range(0, value.shape[1], 128)
    ]
    return parts[0] if len(parts) == 1 else jnp.concatenate(parts, axis=1)


def dot(left, right):
    return jnp.dot(left, right, preferred_element_type=jnp.float32)


def dot_nt(left, right):
    return lax.dot_general(
        left, right, (((1,), (1,)), ((), ())), preferred_element_type=jnp.float32
    )


def forward_kernel(
    fields_far, depth_far, second_far, first_far, out, fields, depth, second, first, sems
):
    half = TX // 2
    pairs = [
        (depth_far, depth),
        (fields_far.at[:half], fields.at[:half]),
        (fields_far.at[half:], fields.at[half:]),
        (second_far, second),
        (first_far, first),
    ]
    copies = [
        pltpu.make_async_copy(here, there, sems.at[n]) for n, (here, there) in enumerate(pairs)
    ]
    for n, copy in enumerate(copies):
        copy.start(priority=0 if n < 3 else 1)
    copies[0].wait()
    amplitudes = []
    for part in range(2):
        copies[1 + part].wait()
        amplitude = None
        for p in range(YL // 2):
            left = jnp.concatenate(
                [
                    fields[part * half : (part + 1) * half, :, 2 * p + h].reshape(-1, Z)
                    for h in range(2)
                ],
                axis=1,
            )
            term = dot(left, depth[p * 2 * Z : (p + 1) * 2 * Z, :])
            amplitude = term if amplitude is None else amplitude + term
        amplitudes.append(amplitude.astype(jnp.bfloat16).reshape(half, YH, C, 2 * YL * MZ))
    amplitude = jnp.concatenate(amplitudes, axis=0)
    copies[3].wait()
    along = None
    for h in range(YH):
        term = dot(amplitude[:, h].reshape(TX * C, 256), second[h * 256 : (h + 1) * 256, :])
        along = term if along is None else along + term
    both = jnp.concatenate(
        [along.astype(jnp.bfloat16), turned(along).astype(jnp.bfloat16)], axis=0
    )
    copies[4].wait()
    modes = dot(first[...], both).astype(jnp.bfloat16)
    for j in range(MX):
        for b in range(KB):
            out[j * KB + b] = modes[j * C : (j + 1) * C, b * 128 : (b + 1) * 128]


def prepare_kernel(own, other, out):
    row = lax.broadcasted_iota(jnp.int32, (4 * C, C), 0)
    column = lax.broadcasted_iota(jnp.int32, (4 * C, C), 1)
    for n, source in enumerate((own, other)):
        total = jnp.zeros((4 * C, 128), jnp.float32)
        for d in range(4):
            piece = jnp.concatenate(
                [source[k, r, d] for r in range(2) for k in range(KL)], axis=0
            )
            pick = jnp.where(row == column * 4 + d, 1.0, 0.0).astype(jnp.bfloat16)
            total = total + dot_nt(pick, piece)
        out[n] = total.astype(jnp.bfloat16)


def position_phases():
    at_x = lax.axis_index("gx").astype(jnp.int32)
    at_y = lax.axis_index("gy").astype(jnp.int32)
    freq_x = jnp.where(at_x < 8, at_x, at_x - 16)
    lane = lax.broadcasted_iota(jnp.int32, (64, 128), 1)
    place = lax.broadcasted_iota(jnp.int32, (64, 128), 0)
    freq_y = at_y * KL + ((lane >> 4) & 3)
    freq_y = jnp.where(freq_y < 8, freq_y, freq_y - 16)
    turn = (freq_x * (place >> 2) + freq_y * (place & 3) * 4) & 15
    cosine = jnp.ones((64, 128), jnp.float32)
    sine = jnp.zeros((64, 128), jnp.float32)
    for n in range(1, 16):
        here = turn == n
        cosine = jnp.where(here, math.cos(2.0 * math.pi * n / 16), cosine)
        sine = jnp.where(here, math.sin(2.0 * math.pi * n / 16), sine)
    return cosine, sine


def collect_kernel(parts_far, out, cosine, sine, parts, sems):
    copies = [
        pltpu.make_async_copy(
            parts_far.at[g * 16 : (g + 1) * 16], parts.at[g * 16 : (g + 1) * 16], sems.at[g]
        )
        for g in range(4)
    ]
    for copy in copies:
        copy.start()
    cosine[...], sine[...] = position_phases()
    real = jnp.zeros((C, 128), jnp.float32)
    imag = jnp.zeros((C, 128), jnp.float32)
    for s in range(64):
        if s % 16 == 0:
            copies[s // 16].wait()
        part = parts[s].astype(jnp.float32)
        real = real + part * cosine[s : s + 1, :]
        imag = imag + part * sine[s : s + 1, :]
    total = (real - turned(imag)) * (1.0 / math.sqrt(X * Y * Z))
    out[...] = total


def mix_kernel(total, here, before, after, across, cosine, sine, out):
    row = lax.broadcasted_iota(jnp.int32, (4 * C, C), 0)
    column = lax.broadcasted_iota(jnp.int32, (4 * C, C), 1)
    repeat = jnp.where((row >> 2) == column, 1.0, 0.0).astype(jnp.bfloat16)
    spectrum = dot(repeat, total[...].astype(jnp.bfloat16))
    swapped = pltpu.roll(spectrum, 64, 1)
    lane = lax.broadcasted_iota(jnp.int32, (8, 128), 1)
    row = lax.broadcasted_iota(jnp.int32, (8, 128), 0)

    def mixed_with(weight):
        w = weight.astype(jnp.float32)
        same = jnp.sum((spectrum * w).reshape(16, 8, 128), axis=0)
        cross = jnp.sum((swapped * w).reshape(16, 8, 128), axis=0)
        same = same + pltpu.roll(same, 4, 0)
        cross = cross + pltpu.roll(cross, 4, 0)
        same = same - pltpu.roll(same, 64, 1)
        cross = cross + pltpu.roll(cross, 64, 1)
        return jnp.where(lane < 64, same, cross)

    place = lax.axis_index("col").astype(jnp.int32)
    nearer = (row >> 2) == (place & 1)
    blocks = [jnp.zeros((8, 128), jnp.float32) for _ in range(4)]
    for offset, weight in ((0, here), (3, before), (1, after), (2, across)):
        block = jnp.where(nearer, mixed_with(weight[0]), mixed_with(weight[1]))
        source = ((place >> 1) + offset) & 3
        blocks = [jnp.where(source == i, block, blocks[i]) for i in range(4)]
    mixed = jnp.concatenate(blocks, axis=0)
    mixed_turned = turned(mixed)
    for s in range(64):
        out[s] = (mixed * cosine[s : s + 1, :] + mixed_turned * sine[s : s + 1, :]).astype(
            jnp.bfloat16
        )


def column_of(vector):
    row = lax.broadcasted_iota(jnp.int32, (C, C), 0)
    column = lax.broadcasted_iota(jnp.int32, (C, C), 1)
    spread = jnp.where(row == column, jnp.broadcast_to(vector[...], (C, C)), 0.0)
    return jnp.broadcast_to(jnp.sum(spread, axis=1, keepdims=True), (C, Z))


def inverse_kernel(
    modes, fields, depth, second, first, skip, bias, gain, shift, out, rows, spectral, done, sems
):
    full = jnp.concatenate(
        [
            jnp.concatenate([modes[j * KB + b] for j in range(MX)], axis=0)
            for b in range(KB)
        ],
        axis=1,
    )
    both = dot(first[...], full)
    lines = both[: TX * C] + turned(both[TX * C :])
    lines = lines * (1.0 / math.sqrt(MX * MY * MZ))
    lines = lines.reshape(TX, C, YH * 128)
    lines = lines - jnp.sum(lines, axis=1, keepdims=True) * (1.0 / C)
    lines = lines.reshape(TX * C, YH * 128).astype(jnp.bfloat16)
    rows[...] = dot_nt(lines, second[...]).astype(jnp.bfloat16)
    row = lax.broadcasted_iota(jnp.int32, (YL * C, YL * C), 0)
    column = lax.broadcasted_iota(jnp.int32, (YL * C, YL * C), 1)
    block = (row >> 5) == (column >> 5)
    square = skip[0].astype(jnp.float32)
    square = square - jnp.sum(square, axis=0, keepdims=True) * (1.0 / C)
    wide = jnp.concatenate([square] * YL, axis=1)
    tall = jnp.where(block, jnp.concatenate([wide] * YL, axis=0), 0.0)
    skips = tall.astype(jnp.bfloat16)
    bias = column_of(bias)
    bias = bias - jnp.sum(bias, axis=0, keepdims=True) * (1.0 / C)
    gain = column_of(gain) * math.sqrt(0.5)
    shift = column_of(shift) * math.sqrt(0.5)
    copies = []
    for h in range(YH):
        spectral[h % 2] = dot_nt(rows[:, h * 256 : (h + 1) * 256], depth[...])
        for x in range(0, TX, 2):
            cells = jnp.concatenate(
                [fields[x + i, h].reshape(YL * C, Z) for i in range(2)], axis=1
            )
            skipped = dot(skips, cells)
            for i in range(2):
                for y in range(YL):
                    pre = (
                        spectral[h % 2, (x + i) * C : (x + i + 1) * C, y * Z : (y + 1) * Z]
                        + skipped[y * C : (y + 1) * C, i * Z : (i + 1) * Z]
                        + bias
                    )
                    spread = jnp.sum(pre * pre, axis=0, keepdims=True) * (1.0 / C)
                    normed = pre * lax.rsqrt(spread + norm_eps) * gain + shift
                    half = normed * math.sqrt(0.5)
                    done[h, x + i, y] = (half * lax.erf(normed) + half).astype(jnp.bfloat16)
            copy = pltpu.make_async_copy(
                done.at[h, x : x + 2], out.at[x : x + 2, h], sems.at[h * 4 + x // 2]
            )
            copy.start()
            copies.append(copy)
    for copy in copies:
        copy.wait()


def near(value):
    return pltpu.with_memory_space_constraint(value, pltpu.VMEM)


def far(value):
    return pltpu.with_memory_space_constraint(value, pltpu.HBM)


def local(fields, spectral, skip_weight, skip_bias, norm_gain, norm_shift):
    bf16 = jnp.bfloat16
    hidden = fields.reshape(TX, YH, YL, C, Z)
    depth = jnp.asarray(depth_table(), bf16)
    second = jnp.asarray(second_table(), bf16)
    first_forward, first_backward = first_tables()
    first_forward = jnp.asarray(first_forward, bf16)
    first_backward = jnp.asarray(first_backward, bf16)
    anywhere = pl.BlockSpec(memory_space=pl.ANY)

    raw = spectral[0, 0].transpose(0, 1, 3, 4, 2)
    partner = lax.ppermute(raw, "col", [(i, i ^ 1) for i in range(8)])
    weight = pl.pallas_call(
        prepare_kernel,
        out_shape=jax.ShapeDtypeStruct((2, 128, 128), bf16),
        compiler_params=pltpu.CompilerParams(vmem_limit_bytes=8 << 20),
        name="prepare",
    )(raw, partner)
    around = []
    for step in (4, 2, 6):
        source = weight
        around.append(
            lax.ppermute(source, "col", [(i, (i + step) % 8) for i in range(8)])
        )

    modes, hidden = pl.pallas_call(
        forward_kernel,
        in_specs=[anywhere] * 4,
        out_shape=[
            pltpu.VMEM((64, C, 128), bf16),
            pltpu.VMEM(hidden.shape, bf16),
        ],
        scratch_shapes=[
            pltpu.VMEM(depth.shape, bf16),
            pltpu.VMEM(second.shape, bf16),
            pltpu.VMEM(first_forward.shape, bf16),
            pltpu.SemaphoreType.DMA((5,)),
        ],
        compiler_params=pltpu.CompilerParams(vmem_limit_bytes=20 << 20),
        name="forward",
    )(far(hidden), far(depth), far(second), far(first_forward))
    parts = lax.all_to_all(
        modes, ("gx", "gy"), split_axis=0, concat_axis=0, tiled=True
    )
    total, cosine, sine = pl.pallas_call(
        collect_kernel,
        in_specs=[anywhere],
        scratch_shapes=[pltpu.VMEM((64, C, 128), bf16), pltpu.SemaphoreType.DMA((4,))],
        out_shape=[
            pltpu.VMEM((C, 128), jnp.float32),
            pltpu.VMEM((64, 128), jnp.float32),
            pltpu.VMEM((64, 128), jnp.float32),
        ],
        compiler_params=pltpu.CompilerParams(vmem_limit_bytes=12 << 20),
        name="collect",
    )(far(parts))
    mixed = pl.pallas_call(
        mix_kernel,
        out_shape=pltpu.VMEM((64, C, 128), bf16),
        compiler_params=pltpu.CompilerParams(vmem_limit_bytes=12 << 20),
        name="mix",
    )(total, near(weight), *[near(around[n]) for n in (1, 2, 0)], cosine, sine)
    full = lax.all_to_all(mixed, ("gx", "gy"), split_axis=0, concat_axis=0, tiled=True)
    result = pl.pallas_call(
        inverse_kernel,
        out_shape=jax.ShapeDtypeStruct((TX, YH, YL, C, Z), bf16),
        out_specs=anywhere,
        scratch_shapes=[
            pltpu.VMEM((TX * C, YH * 256), bf16),
            pltpu.VMEM((2, TX * C, YL * Z), jnp.float32),
            pltpu.VMEM((YH, TX, YL, C, Z), bf16),
            pltpu.SemaphoreType.DMA((YH * 4,)),
        ],
        compiler_params=pltpu.CompilerParams(vmem_limit_bytes=24 << 20),
        name="inverse",
    )(
        near(full),
        hidden,
        near(depth),
        near(second),
        near(first_backward),
        skip_weight,
        skip_bias,
        norm_gain,
        norm_shift,
    )
    return result.reshape(1, TX, TY, C, Z)


def solution(mesh):
    placed = (
        P("col", "gx", "gy", None, None),
        P(None, "gx", "gy", None, None, "col", None),
        P(),
        P(),
        P(),
        P(),
    )
    return jax.shard_map(
        local,
        mesh=mesh,
        in_specs=placed,
        out_specs=P("col", "gx", "gy", None, None),
        check_vma=False,
    )
```

```python
import math

import jax
import jax.numpy as jnp
import numpy as np
from jax import lax
from jax.experimental import pallas as pl
from jax.experimental.pallas import tpu as pltpu
from jax.sharding import PartitionSpec as P


X = 128
Y = 128
Z = 128
MX = 16
MY = 16
MZ = 16
C = 32
TX = 8
TY = 32
YH = 4
YL = 8
KB = 4
KL = 4

norm_eps = 1e-05


def signed(count):
    index = np.arange(count)
    return np.where(index < count // 2, index, index - count)


def depth_table():
    phase = 2.0 * np.pi * ((np.arange(Z)[:, None] * np.arange(MZ)[None, :]) % Z) / Z
    parts = np.stack([np.cos(phase), -np.sin(phase)], axis=1)
    full = np.einsum("zrk,ab->azrbk", parts, np.eye(YL))
    return full.reshape(YL * Z, 2 * YL * MZ)


def second_table():
    cells = np.arange(TY)
    phase = 2.0 * np.pi * ((cells[:, None] * signed(MY)[None, :]) % Y) / Y
    cosine, sine = np.cos(phase), np.sin(phase)
    from_real = np.stack([cosine, -sine], axis=-1)
    from_imag = np.stack([sine, cosine], axis=-1)
    both = np.stack([from_real, from_imag], axis=1)
    both = both.reshape(YH, YL, 2, KB, KL, 2)
    full = np.einsum("hlrbkt,vw->hrlvbtkw", both, np.eye(MZ))
    return full.reshape(YH * 2 * YL * MZ, KB * 2 * KL * MZ)


def first_tables():
    cells = np.arange(TX)
    phase = 2.0 * np.pi * ((signed(MX)[:, None] * cells[None, :]) % X) / X
    cosine = np.kron(np.cos(phase), np.eye(C))
    sine = np.kron(np.sin(phase), np.eye(C))
    forward = np.concatenate([cosine, -sine], axis=1)
    backward = np.concatenate([cosine.T, sine.T], axis=0)
    return forward, backward


def turned(value):
    lane = lax.broadcasted_iota(jnp.int32, (1, 128), 1)
    sign = jnp.where(lane < 64, -1.0, 1.0)
    parts = [
        pltpu.roll(value[:, at : at + 128], 64, 1) * sign for at in range(0, value.shape[1], 128)
    ]
    return parts[0] if len(parts) == 1 else jnp.concatenate(parts, axis=1)


def dot(left, right):
    return jnp.dot(left, right, preferred_element_type=jnp.float32)


def dot_nt(left, right):
    return lax.dot_general(
        left, right, (((1,), (1,)), ((), ())), preferred_element_type=jnp.float32
    )


def forward_kernel(
    fields_far, depth_far, second_far, first_far, out, fields, depth, second, first, sems
):
    half = TX // 2
    pairs = [
        (depth_far, depth),
        (fields_far.at[:half], fields.at[:half]),
        (fields_far.at[half:], fields.at[half:]),
        (second_far, second),
        (first_far, first),
    ]
    copies = [
        pltpu.make_async_copy(here, there, sems.at[n]) for n, (here, there) in enumerate(pairs)
    ]
    for n, copy in enumerate(copies):
        copy.start(priority=0 if n < 3 else 1)
    copies[0].wait()
    amplitudes = []
    for part in range(2):
        copies[1 + part].wait()
        amplitude = None
        for p in range(YL // 2):
            left = jnp.concatenate(
                [
                    fields[part * half : (part + 1) * half, :, 2 * p + h].reshape(-1, Z)
                    for h in range(2)
                ],
                axis=1,
            )
            term = dot(left, depth[p * 2 * Z : (p + 1) * 2 * Z, :])
            amplitude = term if amplitude is None else amplitude + term
        amplitudes.append(amplitude.astype(jnp.bfloat16).reshape(half, YH, C, 2 * YL * MZ))
    amplitude = jnp.concatenate(amplitudes, axis=0)
    copies[3].wait()
    along = None
    for h in range(YH):
        term = dot(amplitude[:, h].reshape(TX * C, 256), second[h * 256 : (h + 1) * 256, :])
        along = term if along is None else along + term
    both = jnp.concatenate(
        [along.astype(jnp.bfloat16), turned(along).astype(jnp.bfloat16)], axis=0
    )
    copies[4].wait()
    modes = dot(first[...], both).astype(jnp.bfloat16)
    for j in range(MX):
        for b in range(KB):
            out[j * KB + b] = modes[j * C : (j + 1) * C, b * 128 : (b + 1) * 128]


def prepare_kernel(own, other, out):
    row = lax.broadcasted_iota(jnp.int32, (4 * C, C), 0)
    column = lax.broadcasted_iota(jnp.int32, (4 * C, C), 1)
    for n, source in enumerate((own, other)):
        total = jnp.zeros((4 * C, 128), jnp.float32)
        for d in range(4):
            piece = jnp.concatenate(
                [source[k, r, d] for r in range(2) for k in range(KL)], axis=0
            )
            pick = jnp.where(row == column * 4 + d, 1.0, 0.0).astype(jnp.bfloat16)
            total = total + dot_nt(pick, piece)
        out[n] = total.astype(jnp.bfloat16)


def position_phases():
    at_x = lax.axis_index("gx").astype(jnp.int32)
    at_y = lax.axis_index("gy").astype(jnp.int32)
    freq_x = jnp.where(at_x < 8, at_x, at_x - 16)
    lane = lax.broadcasted_iota(jnp.int32, (64, 128), 1)
    place = lax.broadcasted_iota(jnp.int32, (64, 128), 0)
    freq_y = at_y * KL + ((lane >> 4) & 3)
    freq_y = jnp.where(freq_y < 8, freq_y, freq_y - 16)
    turn = (freq_x * (place >> 2) + freq_y * (place & 3) * 4) & 15
    cosine = jnp.ones((64, 128), jnp.float32)
    sine = jnp.zeros((64, 128), jnp.float32)
    for n in range(1, 16):
        here = turn == n
        cosine = jnp.where(here, math.cos(2.0 * math.pi * n / 16), cosine)
        sine = jnp.where(here, math.sin(2.0 * math.pi * n / 16), sine)
    return cosine, sine


def collect_kernel(parts_far, out, cosine, sine, parts, sems):
    copies = [
        pltpu.make_async_copy(
            parts_far.at[g * 16 : (g + 1) * 16], parts.at[g * 16 : (g + 1) * 16], sems.at[g]
        )
        for g in range(4)
    ]
    for copy in copies:
        copy.start()
    cosine[...], sine[...] = position_phases()
    real = jnp.zeros((C, 128), jnp.float32)
    imag = jnp.zeros((C, 128), jnp.float32)
    for s in range(64):
        if s % 16 == 0:
            copies[s // 16].wait()
        part = parts[s].astype(jnp.float32)
        real = real + part * cosine[s : s + 1, :]
        imag = imag + part * sine[s : s + 1, :]
    total = (real - turned(imag)) * (1.0 / math.sqrt(X * Y * Z))
    out[...] = total


def mix_kernel(total, here, before, after, across, cosine, sine, out):
    row = lax.broadcasted_iota(jnp.int32, (4 * C, C), 0)
    column = lax.broadcasted_iota(jnp.int32, (4 * C, C), 1)
    repeat = jnp.where((row >> 2) == column, 1.0, 0.0).astype(jnp.bfloat16)
    spectrum = dot(repeat, total[...].astype(jnp.bfloat16))
    swapped = pltpu.roll(spectrum, 64, 1)
    lane = lax.broadcasted_iota(jnp.int32, (8, 128), 1)
    row = lax.broadcasted_iota(jnp.int32, (8, 128), 0)

    def mixed_with(weight):
        w = weight.astype(jnp.float32)
        same = jnp.sum((spectrum * w).reshape(16, 8, 128), axis=0)
        cross = jnp.sum((swapped * w).reshape(16, 8, 128), axis=0)
        same = same + pltpu.roll(same, 4, 0)
        cross = cross + pltpu.roll(cross, 4, 0)
        same = same - pltpu.roll(same, 64, 1)
        cross = cross + pltpu.roll(cross, 64, 1)
        return jnp.where(lane < 64, same, cross)

    place = lax.axis_index("col").astype(jnp.int32)
    nearer = (row >> 2) == (place & 1)
    blocks = [jnp.zeros((8, 128), jnp.float32) for _ in range(4)]
    for offset, weight in ((0, here), (3, before), (1, after), (2, across)):
        block = jnp.where(nearer, mixed_with(weight[0]), mixed_with(weight[1]))
        source = ((place >> 1) + offset) & 3
        blocks = [jnp.where(source == i, block, blocks[i]) for i in range(4)]
    mixed = jnp.concatenate(blocks, axis=0)
    mixed_turned = turned(mixed)
    for s in range(64):
        out[s] = (mixed * cosine[s : s + 1, :] + mixed_turned * sine[s : s + 1, :]).astype(
            jnp.bfloat16
        )


def column_of(vector, scale=1.0):
    row = lax.broadcasted_iota(jnp.int32, (C, C), 0)
    column = lax.broadcasted_iota(jnp.int32, (C, C), 1)
    spread = jnp.where(row == column, jnp.broadcast_to(vector[...] * scale, (C, C)), 0.0)
    return jnp.broadcast_to(jnp.sum(spread, axis=1, keepdims=True), (C, Z))


def inverse_kernel(
    modes, fields, depth, second, first, skip, bias_row, gain_row, shift_row,
    out, bias, gain, shift, spectral, done, sems,
):
    full = jnp.concatenate(
        [
            jnp.concatenate([modes[j * KB + b] for j in range(MX)], axis=0)
            for b in range(KB)
        ],
        axis=1,
    )
    both = dot(first[...], full)
    lines = both[: TX * C] + turned(both[TX * C :])
    lines = lines * (1.0 / math.sqrt(MX * MY * MZ))
    lines = lines.reshape(TX, C, YH * 128)
    lines = lines - jnp.sum(lines, axis=1, keepdims=True) * (1.0 / C)
    lines = lines.reshape(TX * C, YH * 128).astype(jnp.bfloat16)
    row = lax.broadcasted_iota(jnp.int32, (YL * C, YL * C), 0)
    column = lax.broadcasted_iota(jnp.int32, (YL * C, YL * C), 1)
    block = (row >> 5) == (column >> 5)
    square = skip[0].astype(jnp.float32)
    square = square - jnp.sum(square, axis=0, keepdims=True) * (1.0 / C)
    wide = jnp.concatenate([square] * YL, axis=1)
    tall = jnp.where(block, jnp.concatenate([wide] * YL, axis=0), 0.0)
    skips = tall.astype(jnp.bfloat16)
    offset = column_of(bias_row)
    bias[...] = offset - jnp.sum(offset, axis=0, keepdims=True) * (1.0 / C)
    gain[...] = column_of(gain_row, math.sqrt(0.5 * C))
    shift[...] = column_of(shift_row, math.sqrt(0.5))
    copies = []
    for h in range(YH):
        rows = dot_nt(lines, second[h * 256 : (h + 1) * 256, :]).astype(jnp.bfloat16)
        spectral[h % 2] = dot_nt(rows, depth[...])
        for x in range(0, TX, 2):
            cells = jnp.concatenate(
                [fields[x + i, h].reshape(YL * C, Z) for i in range(2)], axis=1
            )
            skipped = dot(skips, cells)
            for i in range(2):
                for y in range(YL):
                    pre = (
                        spectral[h % 2, (x + i) * C : (x + i + 1) * C, y * Z : (y + 1) * Z]
                        + skipped[y * C : (y + 1) * C, i * Z : (i + 1) * Z]
                        + bias[...]
                    )
                    spread = jnp.sum(pre * pre, axis=0, keepdims=True)
                    normed = pre * lax.rsqrt(spread + C * norm_eps) * gain[...] + shift[...]
                    half = normed * math.sqrt(0.5)
                    done[h, x + i, y] = (half * lax.erf(normed) + half).astype(jnp.bfloat16)
            copy = pltpu.make_async_copy(
                done.at[h, x : x + 2], out.at[x : x + 2, h], sems.at[h * 4 + x // 2]
            )
            copy.start()
            copies.append(copy)
    for copy in copies:
        copy.wait()


def near(value):
    return pltpu.with_memory_space_constraint(value, pltpu.VMEM)


def far(value):
    return pltpu.with_memory_space_constraint(value, pltpu.HBM)


def local(fields, spectral, skip_weight, skip_bias, norm_gain, norm_shift):
    bf16 = jnp.bfloat16
    hidden = fields.reshape(TX, YH, YL, C, Z)
    depth = jnp.asarray(depth_table(), bf16)
    second = jnp.asarray(second_table(), bf16)
    first_forward, first_backward = first_tables()
    first_forward = jnp.asarray(first_forward, bf16)
    first_backward = jnp.asarray(first_backward, bf16)
    anywhere = pl.BlockSpec(memory_space=pl.ANY)

    raw = spectral[0, 0].transpose(0, 1, 3, 4, 2)
    partner = lax.ppermute(raw, "col", [(i, i ^ 1) for i in range(8)])
    weight = pl.pallas_call(
        prepare_kernel,
        out_shape=jax.ShapeDtypeStruct((2, 128, 128), bf16),
        compiler_params=pltpu.CompilerParams(vmem_limit_bytes=8 << 20),
        name="prepare",
    )(raw, partner)
    around = []
    for step in (4, 2, 6):
        source = weight
        around.append(
            lax.ppermute(source, "col", [(i, (i + step) % 8) for i in range(8)])
        )

    modes, hidden = pl.pallas_call(
        forward_kernel,
        in_specs=[anywhere] * 4,
        out_shape=[
            pltpu.VMEM((64, C, 128), bf16),
            pltpu.VMEM(hidden.shape, bf16),
        ],
        scratch_shapes=[
            pltpu.VMEM(depth.shape, bf16),
            pltpu.VMEM(second.shape, bf16),
            pltpu.VMEM(first_forward.shape, bf16),
            pltpu.SemaphoreType.DMA((5,)),
        ],
        compiler_params=pltpu.CompilerParams(vmem_limit_bytes=20 << 20),
        name="forward",
    )(far(hidden), far(depth), far(second), far(first_forward))
    parts = lax.all_to_all(
        modes, ("gx", "gy"), split_axis=0, concat_axis=0, tiled=True
    )
    total, cosine, sine = pl.pallas_call(
        collect_kernel,
        in_specs=[anywhere],
        scratch_shapes=[pltpu.VMEM((64, C, 128), bf16), pltpu.SemaphoreType.DMA((4,))],
        out_shape=[
            pltpu.VMEM((C, 128), jnp.float32),
            pltpu.VMEM((64, 128), jnp.float32),
            pltpu.VMEM((64, 128), jnp.float32),
        ],
        compiler_params=pltpu.CompilerParams(vmem_limit_bytes=12 << 20),
        name="collect",
    )(far(parts))
    mixed = pl.pallas_call(
        mix_kernel,
        out_shape=pltpu.VMEM((64, C, 128), bf16),
        compiler_params=pltpu.CompilerParams(vmem_limit_bytes=12 << 20),
        name="mix",
    )(total, near(weight), *[near(around[n]) for n in (1, 2, 0)], cosine, sine)
    full = lax.all_to_all(mixed, ("gx", "gy"), split_axis=0, concat_axis=0, tiled=True)
    result = pl.pallas_call(
        inverse_kernel,
        out_shape=jax.ShapeDtypeStruct((TX, YH, YL, C, Z), bf16),
        out_specs=anywhere,
        scratch_shapes=[
            pltpu.VMEM((C, Z), jnp.float32),
            pltpu.VMEM((C, Z), jnp.float32),
            pltpu.VMEM((C, Z), jnp.float32),
            pltpu.VMEM((2, TX * C, YL * Z), jnp.float32),
            pltpu.VMEM((YH, TX, YL, C, Z), bf16),
            pltpu.SemaphoreType.DMA((YH * 4,)),
        ],
        compiler_params=pltpu.CompilerParams(vmem_limit_bytes=24 << 20),
        name="inverse",
    )(
        near(full),
        hidden,
        near(depth),
        near(second),
        near(first_backward),
        skip_weight,
        skip_bias,
        norm_gain,
        norm_shift,
    )
    return result.reshape(1, TX, TY, C, Z)


def solution(mesh):
    placed = (
        P("col", "gx", "gy", None, None),
        P(None, "gx", "gy", None, None, "col", None),
        P(),
        P(),
        P(),
        P(),
    )
    return jax.shard_map(
        local,
        mesh=mesh,
        in_specs=placed,
        out_specs=P("col", "gx", "gy", None, None),
        check_vma=False,
    )
```

```python
import math

import jax
import jax.numpy as jnp
import numpy as np
from jax import lax
from jax.experimental import pallas as pl
from jax.experimental.pallas import tpu as pltpu
from jax.sharding import PartitionSpec as P


X = 128
Y = 128
Z = 128
MX = 16
MY = 16
MZ = 16
C = 32
TX = 8
TY = 32
YH = 4
YL = 8
KB = 4
KL = 4

norm_eps = 1e-05


def signed(count):
    index = np.arange(count)
    return np.where(index < count // 2, index, index - count)


def depth_table():
    phase = 2.0 * np.pi * ((np.arange(Z)[:, None] * np.arange(MZ)[None, :]) % Z) / Z
    parts = np.stack([np.cos(phase), -np.sin(phase)], axis=1)
    full = np.einsum("zrk,ab->azrbk", parts, np.eye(YL))
    return full.reshape(YL * Z, 2 * YL * MZ)


def second_table():
    cells = np.arange(TY)
    phase = 2.0 * np.pi * ((cells[:, None] * signed(MY)[None, :]) % Y) / Y
    cosine, sine = np.cos(phase), np.sin(phase)
    from_real = np.stack([cosine, -sine], axis=-1)
    from_imag = np.stack([sine, cosine], axis=-1)
    both = np.stack([from_real, from_imag], axis=1)
    both = both.reshape(YH, YL, 2, KB, KL, 2)
    full = np.einsum("hlrbkt,vw->hrlvbtkw", both, np.eye(MZ))
    return full.reshape(YH * 2 * YL * MZ, KB * 2 * KL * MZ)


def first_tables():
    cells = np.arange(TX)
    phase = 2.0 * np.pi * ((signed(MX)[:, None] * cells[None, :]) % X) / X
    cosine = np.kron(np.cos(phase), np.eye(C))
    sine = np.kron(np.sin(phase), np.eye(C))
    forward = np.concatenate([cosine, -sine], axis=1)
    backward = np.concatenate([cosine.T, sine.T], axis=0)
    return forward, backward


def turned(value):
    lane = lax.broadcasted_iota(jnp.int32, (1, 128), 1)
    sign = jnp.where(lane < 64, -1.0, 1.0)
    parts = [
        pltpu.roll(value[:, at : at + 128], 64, 1) * sign for at in range(0, value.shape[1], 128)
    ]
    return parts[0] if len(parts) == 1 else jnp.concatenate(parts, axis=1)


def dot(left, right):
    return jnp.dot(left, right, preferred_element_type=jnp.float32)


def dot_nt(left, right):
    return lax.dot_general(
        left, right, (((1,), (1,)), ((), ())), preferred_element_type=jnp.float32
    )


def forward_kernel(
    fields_far, depth_far, second_far, first_far, out, fields, depth, second, first, sems
):
    half = TX // 2
    pairs = [
        (depth_far, depth),
        (fields_far.at[:half], fields.at[:half]),
        (fields_far.at[half:], fields.at[half:]),
        (second_far, second),
        (first_far, first),
    ]
    copies = [
        pltpu.make_async_copy(here, there, sems.at[n]) for n, (here, there) in enumerate(pairs)
    ]
    for n, copy in enumerate(copies):
        copy.start(priority=0 if n < 3 else 1)
    copies[0].wait()
    amplitudes = []
    for part in range(2):
        copies[1 + part].wait()
        amplitude = None
        for p in range(YL // 2):
            left = jnp.concatenate(
                [
                    fields[part * half : (part + 1) * half, :, 2 * p + h].reshape(-1, Z)
                    for h in range(2)
                ],
                axis=1,
            )
            term = dot(left, depth[p * 2 * Z : (p + 1) * 2 * Z, :])
            amplitude = term if amplitude is None else amplitude + term
        amplitudes.append(amplitude.astype(jnp.bfloat16).reshape(half, YH, C, 2 * YL * MZ))
    amplitude = jnp.concatenate(amplitudes, axis=0)
    copies[3].wait()
    along = None
    for h in range(YH):
        term = dot(amplitude[:, h].reshape(TX * C, 256), second[h * 256 : (h + 1) * 256, :])
        along = term if along is None else along + term
    both = jnp.concatenate(
        [along.astype(jnp.bfloat16), turned(along).astype(jnp.bfloat16)], axis=0
    )
    copies[4].wait()
    modes = dot(first[...], both).astype(jnp.bfloat16)
    for j in range(MX):
        for b in range(KB):
            out[j * KB + b] = modes[j * C : (j + 1) * C, b * 128 : (b + 1) * 128]


def prepare_kernel(own, other, out):
    row = lax.broadcasted_iota(jnp.int32, (4 * C, C), 0)
    column = lax.broadcasted_iota(jnp.int32, (4 * C, C), 1)
    for n, source in enumerate((own, other)):
        total = jnp.zeros((4 * C, 128), jnp.float32)
        for d in range(4):
            piece = jnp.concatenate(
                [source[k, r, d] for r in range(2) for k in range(KL)], axis=0
            )
            pick = jnp.where(row == column * 4 + d, 1.0, 0.0).astype(jnp.bfloat16)
            total = total + dot_nt(pick, piece)
        out[n] = total.astype(jnp.bfloat16)


def position_phases():
    at_x = lax.axis_index("gx").astype(jnp.int32)
    at_y = lax.axis_index("gy").astype(jnp.int32)
    freq_x = jnp.where(at_x < 8, at_x, at_x - 16)
    lane = lax.broadcasted_iota(jnp.int32, (64, 128), 1)
    place = lax.broadcasted_iota(jnp.int32, (64, 128), 0)
    freq_y = at_y * KL + ((lane >> 4) & 3)
    freq_y = jnp.where(freq_y < 8, freq_y, freq_y - 16)
    turn = (freq_x * (place >> 2) + freq_y * (place & 3) * 4) & 15
    cosine = jnp.ones((64, 128), jnp.float32)
    sine = jnp.zeros((64, 128), jnp.float32)
    for n in range(1, 16):
        here = turn == n
        cosine = jnp.where(here, math.cos(2.0 * math.pi * n / 16), cosine)
        sine = jnp.where(here, math.sin(2.0 * math.pi * n / 16), sine)
    return cosine, sine


def collect_kernel(parts_far, out, cosine, sine, parts, sems):
    copies = [
        pltpu.make_async_copy(
            parts_far.at[g * 8 : (g + 1) * 8], parts.at[g * 8 : (g + 1) * 8], sems.at[g]
        )
        for g in range(8)
    ]
    for copy in copies:
        copy.start()
    cosine[...], sine[...] = position_phases()
    real = jnp.zeros((C, 128), jnp.float32)
    imag = jnp.zeros((C, 128), jnp.float32)
    for s in range(64):
        if s % 8 == 0:
            copies[s // 8].wait()
        part = parts[s].astype(jnp.float32)
        real = real + part * cosine[s : s + 1, :]
        imag = imag + part * sine[s : s + 1, :]
    total = (real - turned(imag)) * (1.0 / math.sqrt(X * Y * Z))
    out[...] = total


def mix_kernel(total, here, before, after, across, cosine, sine, out):
    row = lax.broadcasted_iota(jnp.int32, (4 * C, C), 0)
    column = lax.broadcasted_iota(jnp.int32, (4 * C, C), 1)
    repeat = jnp.where((row >> 2) == column, 1.0, 0.0).astype(jnp.bfloat16)
    spectrum = dot(repeat, total[...].astype(jnp.bfloat16))
    swapped = pltpu.roll(spectrum, 64, 1)
    lane = lax.broadcasted_iota(jnp.int32, (8, 128), 1)
    row = lax.broadcasted_iota(jnp.int32, (8, 128), 0)

    def mixed_with(weight):
        w = weight.astype(jnp.float32)
        same = jnp.sum((spectrum * w).reshape(16, 8, 128), axis=0)
        cross = jnp.sum((swapped * w).reshape(16, 8, 128), axis=0)
        same = same + pltpu.roll(same, 4, 0)
        cross = cross + pltpu.roll(cross, 4, 0)
        same = same - pltpu.roll(same, 64, 1)
        cross = cross + pltpu.roll(cross, 64, 1)
        return jnp.where(lane < 64, same, cross)

    place = lax.axis_index("col").astype(jnp.int32)
    nearer = (row >> 2) == (place & 1)
    blocks = [jnp.zeros((8, 128), jnp.float32) for _ in range(4)]
    for offset, weight in ((0, here), (3, before), (1, after), (2, across)):
        block = jnp.where(nearer, mixed_with(weight[0]), mixed_with(weight[1]))
        source = ((place >> 1) + offset) & 3
        blocks = [jnp.where(source == i, block, blocks[i]) for i in range(4)]
    mixed = jnp.concatenate(blocks, axis=0)
    mixed_turned = turned(mixed)
    for s in range(64):
        out[s] = (mixed * cosine[s : s + 1, :] + mixed_turned * sine[s : s + 1, :]).astype(
            jnp.bfloat16
        )


def column_of(vector, scale=1.0):
    row = lax.broadcasted_iota(jnp.int32, (C, C), 0)
    column = lax.broadcasted_iota(jnp.int32, (C, C), 1)
    spread = jnp.where(row == column, jnp.broadcast_to(vector[...] * scale, (C, C)), 0.0)
    return jnp.broadcast_to(jnp.sum(spread, axis=1, keepdims=True), (C, Z))


def inverse_kernel(
    modes, fields, depth, second, first, skip, bias_row, gain_row, shift_row,
    out, bias, gain, shift, spectral, done, sems,
):
    full = jnp.concatenate(
        [
            jnp.concatenate([modes[j * KB + b] for j in range(MX)], axis=0)
            for b in range(KB)
        ],
        axis=1,
    )
    both = dot(first[...], full)
    lines = both[: TX * C] + turned(both[TX * C :])
    lines = lines * (1.0 / math.sqrt(MX * MY * MZ))
    lines = lines.reshape(TX, C, YH * 128)
    lines = lines - jnp.sum(lines, axis=1, keepdims=True) * (1.0 / C)
    lines = lines.reshape(TX * C, YH * 128).astype(jnp.bfloat16)
    row = lax.broadcasted_iota(jnp.int32, (YL * C, YL * C), 0)
    column = lax.broadcasted_iota(jnp.int32, (YL * C, YL * C), 1)
    block = (row >> 5) == (column >> 5)
    square = skip[0].astype(jnp.float32)
    square = square - jnp.sum(square, axis=0, keepdims=True) * (1.0 / C)
    wide = jnp.concatenate([square] * YL, axis=1)
    tall = jnp.where(block, jnp.concatenate([wide] * YL, axis=0), 0.0)
    skips = tall.astype(jnp.bfloat16)
    offset = column_of(bias_row)
    bias[...] = offset - jnp.sum(offset, axis=0, keepdims=True) * (1.0 / C)
    gain[...] = column_of(gain_row, math.sqrt(0.5 * C))
    shift[...] = column_of(shift_row, math.sqrt(0.5))
    copies = []
    for h in range(YH):
        rows = dot_nt(lines, second[h * 256 : (h + 1) * 256, :]).astype(jnp.bfloat16)
        spectral[h % 2] = dot_nt(rows, depth[...])
        for x in range(0, TX, 2):
            cells = jnp.concatenate(
                [fields[x + i, h].reshape(YL * C, Z) for i in range(2)], axis=1
            )
            skipped = dot(skips, cells)
            for i in range(2):
                for y in range(YL):
                    pre = (
                        spectral[h % 2, (x + i) * C : (x + i + 1) * C, y * Z : (y + 1) * Z]
                        + skipped[y * C : (y + 1) * C, i * Z : (i + 1) * Z]
                        + bias[...]
                    )
                    spread = jnp.sum(pre * pre, axis=0, keepdims=True)
                    normed = pre * lax.rsqrt(spread + C * norm_eps) * gain[...] + shift[...]
                    half = normed * math.sqrt(0.5)
                    done[h, x + i, y] = (half * lax.erf(normed) + half).astype(jnp.bfloat16)
                copy = pltpu.make_async_copy(
                    done.at[h, x + i], out.at[x + i, h], sems.at[h * TX + x + i]
                )
                copy.start()
                copies.append(copy)
    for copy in copies:
        copy.wait()


def near(value):
    return pltpu.with_memory_space_constraint(value, pltpu.VMEM)


def far(value):
    return pltpu.with_memory_space_constraint(value, pltpu.HBM)


def local(fields, spectral, skip_weight, skip_bias, norm_gain, norm_shift):
    bf16 = jnp.bfloat16
    hidden = fields.reshape(TX, YH, YL, C, Z)
    depth = jnp.asarray(depth_table(), bf16)
    second = jnp.asarray(second_table(), bf16)
    first_forward, first_backward = first_tables()
    first_forward = jnp.asarray(first_forward, bf16)
    first_backward = jnp.asarray(first_backward, bf16)
    anywhere = pl.BlockSpec(memory_space=pl.ANY)

    raw = spectral[0, 0].transpose(0, 1, 3, 4, 2)
    partner = lax.ppermute(raw, "col", [(i, i ^ 1) for i in range(8)])
    weight = pl.pallas_call(
        prepare_kernel,
        out_shape=jax.ShapeDtypeStruct((2, 128, 128), bf16),
        compiler_params=pltpu.CompilerParams(vmem_limit_bytes=8 << 20),
        name="prepare",
    )(raw, partner)
    around = []
    for step in (4, 2, 6):
        source = weight
        around.append(
            lax.ppermute(source, "col", [(i, (i + step) % 8) for i in range(8)])
        )

    modes, hidden = pl.pallas_call(
        forward_kernel,
        in_specs=[anywhere] * 4,
        out_shape=[
            pltpu.VMEM((64, C, 128), bf16),
            pltpu.VMEM(hidden.shape, bf16),
        ],
        scratch_shapes=[
            pltpu.VMEM(depth.shape, bf16),
            pltpu.VMEM(second.shape, bf16),
            pltpu.VMEM(first_forward.shape, bf16),
            pltpu.SemaphoreType.DMA((5,)),
        ],
        compiler_params=pltpu.CompilerParams(vmem_limit_bytes=20 << 20),
        name="forward",
    )(far(hidden), far(depth), far(second), far(first_forward))
    parts = lax.all_to_all(
        modes, ("gx", "gy"), split_axis=0, concat_axis=0, tiled=True
    )
    total, cosine, sine = pl.pallas_call(
        collect_kernel,
        in_specs=[anywhere],
        scratch_shapes=[pltpu.VMEM((64, C, 128), bf16), pltpu.SemaphoreType.DMA((8,))],
        out_shape=[
            pltpu.VMEM((C, 128), jnp.float32),
            pltpu.VMEM((64, 128), jnp.float32),
            pltpu.VMEM((64, 128), jnp.float32),
        ],
        compiler_params=pltpu.CompilerParams(vmem_limit_bytes=12 << 20),
        name="collect",
    )(far(parts))
    mixed = pl.pallas_call(
        mix_kernel,
        out_shape=pltpu.VMEM((64, C, 128), bf16),
        compiler_params=pltpu.CompilerParams(vmem_limit_bytes=12 << 20),
        name="mix",
    )(total, near(weight), *[near(around[n]) for n in (1, 2, 0)], cosine, sine)
    full = lax.all_to_all(mixed, ("gx", "gy"), split_axis=0, concat_axis=0, tiled=True)
    result = pl.pallas_call(
        inverse_kernel,
        out_shape=jax.ShapeDtypeStruct((TX, YH, YL, C, Z), bf16),
        out_specs=anywhere,
        scratch_shapes=[
            pltpu.VMEM((C, Z), jnp.float32),
            pltpu.VMEM((C, Z), jnp.float32),
            pltpu.VMEM((C, Z), jnp.float32),
            pltpu.VMEM((2, TX * C, YL * Z), jnp.float32),
            pltpu.VMEM((YH, TX, YL, C, Z), bf16),
            pltpu.SemaphoreType.DMA((YH * TX,)),
        ],
        compiler_params=pltpu.CompilerParams(vmem_limit_bytes=24 << 20),
        name="inverse",
    )(
        near(full),
        hidden,
        near(depth),
        near(second),
        near(first_backward),
        skip_weight,
        skip_bias,
        norm_gain,
        norm_shift,
    )
    return result.reshape(1, TX, TY, C, Z)


def solution(mesh):
    placed = (
        P("col", "gx", "gy", None, None),
        P(None, "gx", "gy", None, None, "col", None),
        P(),
        P(),
        P(),
        P(),
    )
    return jax.shard_map(
        local,
        mesh=mesh,
        in_specs=placed,
        out_specs=P("col", "gx", "gy", None, None),
        check_vma=False,
    )
```
